256 devices in a mesh: leaf: 64 (over y, z, core), grid: 4 (over x).
Axes of the slice: x: 4, y: 4, z: 8, core: 2. Of those that a mesh axis runs over, the one named last changes fastest.
Arguments:
- source_leaf: float32 [8, 32768], P(None, ('leaf', 'grid')), may hold values from -6 to 6
- block_leaf: float32 [32768, 128], P(('leaf', 'grid')), may hold values from -0.5 to 0.5
- expand_leaf: float32 [32768, 128], P(('leaf', 'grid')), may hold values from -0.5 to 0.5
- basis_leaf: float32 [32768, 256], P(('leaf', 'grid')), may hold values from -0.25 to 0.25
- pivot_leaf: float32 [32768], P(('leaf', 'grid')), may hold values from -2 to 2
- couple_leaf: float32 [65536, 128], P(('leaf', 'grid')), may hold values from -0.5 to 0.5
- ranks_leaf: int32 [64, 2], replicated, may hold values from 32 to 128
- targets_leaf: int32 [65536], P(('leaf', 'grid')), may hold values from 0 to 16383, as said below
- source_middle: float32 [8, 32768], P(None, ('leaf', 'grid')), may hold values from -6 to 6
- block_middle: float32 [32768, 128], P(('leaf', 'grid')), may hold values from -0.5 to 0.5
- expand_middle: float32 [32768, 128], P(('leaf', 'grid')), may hold values from -0.5 to 0.5
- basis_middle: float32 [32768, 256], P(('leaf', 'grid')), may hold values from -0.0625 to 0.0625
- pivot_middle: float32 [32768], P(('leaf', 'grid')), may hold values from -2 to 2
- couple_middle: float32 [32768, 128], P(('leaf', 'grid')), may hold values from -0.5 to 0.5
- ranks_middle: int32 [4, 2], replicated, may hold values from 32 to 128
- targets_middle: int32 [32768], P(('leaf', 'grid')), may hold values from 0 to 32767, as said below
- source_upper: float32 [8, 32768], P(None, ('leaf', 'grid')), may hold values from -6 to 6
- block_upper: float32 [32768, 128], P(('leaf', 'grid')), may hold values from -0.5 to 0.5
- expand_upper: float32 [32768, 128], P(('leaf', 'grid')), may hold values from -0.5 to 0.5
- basis_upper: float32 [32768, 256], P(('leaf', 'grid')), may hold values from -0.046875 to 0.046875
- pivot_upper: float32 [32768], P(('leaf', 'grid')), may hold values from -2 to 2
- couple_upper: float32 [32768, 128], P(('leaf', 'grid')), may hold values from -0.5 to 0.5
- ranks_upper: int32 [2, 2], replicated, may hold values from 32 to 128
- targets_upper: int32 [32768], P(('leaf', 'grid')), may hold values from 0 to 32767, as said below
- source_root: float32 [8, 32768], P(None, ('leaf', 'grid')), may hold values from -6 to 6
- block_root: float32 [32768, 128], P(('leaf', 'grid')), may hold values from -0.5 to 0.5
- expand_root: float32 [32768, 128], P(('leaf', 'grid')), may hold values from -0.5 to 0.5
- basis_root: float32 [32768, 256], P(('leaf', 'grid')), may hold values from -0.03125 to 0.03125
- pivot_root: float32 [32768], P(('leaf', 'grid')), may hold values from -2 to 2
- ranks_root: int32 [1, 2], replicated, may hold values from 32 to 128
Outputs:
- answer_leaf: float32 [8, 32768], P(None, ('leaf', 'grid'))
- answer_middle: float32 [8, 32768], P(None, ('leaf', 'grid'))
- answer_upper: float32 [8, 32768], P(None, ('leaf', 'grid'))
- answer_root: float32 [8, 32768], P(None, ('leaf', 'grid'))
The draws below stay inside these ranges and needn't reach their ends.
Inputs may be any that keep to these rules, and one draw needn't show every extreme that they name: `targets_leaf`: within one leaf front the 1024 entries are distinct; each names a row of the parent front's row vector of 16384 rows. Split that vector's separator part and its update part each evenly, in order, over the parent's devices (leaf then grid); then the rows of one device name at most 4 rows held by any one of them, and exactly that many for some. `targets_middle`: within one middle front the entries are distinct; each names a row of the parent front's row vector of 32768 rows. Split likewise over the parent's devices, the rows of one device name at most 1 row held by any one of them, and exactly that many for some. `targets_upper`: within one upper front the entries are distinct; each names a row of the root separator. Split evenly in order over all devices, the rows of one device name at most 1 row held by any one of them, and exactly that many for some.
All inputs are finite; a program needn't handle non-finite values.
Results may differ from the reference program's by a relative error of at most 0.0003.
Values sent between devices are 32-bit elements; how exact they have to be, the bound alone decides.
No kernel may reach another device: no remote copies, remote signals or barrier semaphores. Data moves between devices by JAX's collectives and lax.ppermute only.
A program may use at most 128 MiB of HBM per device.

```python
import jax
import jax.numpy as jnp
from jax import lax

RHS_COUNT = 8
BLOCK = 128
RANK = 128
TOP_ROWS = 128
SEP_LEAF = 512
UPD_LEAF = 1024
SEP_MID = 8192
SEP_UP = 16384
SEP_ROOT = 32768
N_LEAF = 64
N_GRID = 4


def pick_rows(key, salt, fronts, count, owners, width, pieces, sep_rows):
    base = jax.random.fold_in(key, salt)
    slots_each = pieces * width

    def one_front(front):
        fkey = jax.random.fold_in(base, front)
        order = jax.random.permutation(jax.random.fold_in(fkey, 1), owners)
        slot_keys = jax.vmap(lambda owner: jax.random.fold_in(jax.random.fold_in(fkey, 2), owner))(jnp.arange(owners, dtype=jnp.int32))
        slot_order = jax.vmap(lambda one: jax.random.permutation(one, slots_each))(slot_keys)
        rows = jnp.arange(count, dtype=jnp.int32)
        owner = order[rows % owners]
        slot = slot_order[owner, rows // owners]
        return slot // width * sep_rows + owner * width + slot % width
    picked = jax.vmap(one_front)(jnp.arange(fronts, dtype=jnp.int32))
    return picked.reshape(-1).astype(jnp.int32)


def draw_targets_leaf(key, part):
    return pick_rows(key, 11, N_LEAF, UPD_LEAF, N_LEAF * N_GRID // 4, TOP_ROWS, 2, SEP_MID)


def draw_targets_middle(key, part):
    return pick_rows(key, 12, 4, SEP_MID, N_LEAF * N_GRID // 2, TOP_ROWS, 2, SEP_UP)


def draw_targets_upper(key, part):
    return pick_rows(key, 13, 2, SEP_UP, N_LEAF * N_GRID, TOP_ROWS, 1, SEP_ROOT)


def set_ends(array, own_key, low, top_value):
    longest = array.shape.index(max(array.shape))
    spots = []
    for shift in (0, 1):
        where = [jax.random.randint(jax.random.fold_in(own_key, axis), (), 0, length) for axis, length in enumerate(array.shape)]
        where[longest] = (where[longest] + shift) % array.shape[longest]
        spots.append(tuple(where))
    return array.at[spots[0]].set(low).at[spots[1]].set(top_value)


def level_of(rng, dims, shards, least, high):
    def one(position, blocks):
        heights = jax.random.uniform(jax.random.fold_in(jax.random.fold_in(rng, 6), position), (blocks,), jnp.float32, least / len(shards), high / len(shards))
        return jnp.repeat(jnp.exp(heights), dims[position] // blocks).reshape((-1,) + (1,) * (len(dims) - position - 1))

    factor_of = one(*shards[0])
    for cut in shards[1:]:
        factor_of = factor_of * one(*cut)
    return factor_of


def centred(key, dims, scale, limit, shards=(), held_as=jnp.bfloat16):
    factor_of = level_of(key, dims, shards, -0.22, 0.18) if shards else 1.0
    values = jax.random.normal(key, dims, jnp.float32) * scale * factor_of
    return jnp.minimum(jnp.maximum(values, -limit), limit).astype(held_as)


def setup_inputs(seed: int = 0) -> dict:
    key_list = jax.random.split(jax.random.key(seed), 31)
    return {
        "source_leaf": centred(key_list[0], (RHS_COUNT, N_LEAF * SEP_LEAF), 1.0, 6.0, ((1, 256),), jnp.float32),
        "block_leaf": centred(key_list[1], (N_LEAF * SEP_LEAF, BLOCK), BLOCK ** -0.5, 0.5, ((0, 256),), jnp.float32),
        "expand_leaf": centred(key_list[2], (N_LEAF * SEP_LEAF, RANK), RANK ** -0.5, 0.5, ((0, 256),), jnp.float32),
        "basis_leaf": centred(key_list[3], (N_LEAF * SEP_LEAF, 2 * RANK), SEP_LEAF ** -0.5, 0.25, ((0, 256),), jnp.float32),
        "pivot_leaf": jnp.clip(jax.random.uniform(key_list[4], (N_LEAF * SEP_LEAF,), jnp.float32, -2.0, 2.0) * level_of(key_list[4], (N_LEAF * SEP_LEAF,), ((0, 256),), -0.4, 0.0), -2.0, 2.0),
        "couple_leaf": centred(key_list[5], (N_LEAF * UPD_LEAF, RANK), RANK ** -0.5, 0.5, ((0, 256),), jnp.float32),
        "ranks_leaf": set_ends(jax.random.randint(key_list[6], (N_LEAF, 2), RANK // 4, RANK + 1), jax.random.fold_in(key_list[6], 1), RANK // 4, RANK).astype(jnp.int32),
        "targets_leaf": draw_targets_leaf(jax.random.fold_in(key_list[30], 71), 0),
        "source_middle": centred(key_list[8], (RHS_COUNT, 4 * SEP_MID), 1.0, 6.0, ((1, 256),), jnp.float32),
        "block_middle": centred(key_list[9], (4 * SEP_MID, BLOCK), BLOCK ** -0.5, 0.5, ((0, 256),), jnp.float32),
        "expand_middle": centred(key_list[10], (4 * SEP_MID, RANK), RANK ** -0.5, 0.5, ((0, 256),), jnp.float32),
        "basis_middle": centred(key_list[11], (4 * SEP_MID, 2 * RANK), SEP_MID ** -0.5, 0.0625, ((0, 256),), jnp.float32),
        "pivot_middle": jnp.clip(jax.random.uniform(key_list[12], (4 * SEP_MID,), jnp.float32, -2.0, 2.0) * level_of(key_list[12], (4 * SEP_MID,), ((0, 256),), -0.4, 0.0), -2.0, 2.0),
        "couple_middle": centred(key_list[13], (4 * SEP_MID, RANK), RANK ** -0.5, 0.5, ((0, 256),), jnp.float32),
        "ranks_middle": set_ends(jax.random.randint(key_list[14], (4, 2), RANK // 4, RANK + 1), jax.random.fold_in(key_list[14], 1), RANK // 4, RANK).astype(jnp.int32),
        "targets_middle": draw_targets_middle(jax.random.fold_in(key_list[30], 71), 0),
        "source_upper": centred(key_list[16], (RHS_COUNT, 2 * SEP_UP), 1.0, 6.0, ((1, 256),), jnp.float32),
        "block_upper": centred(key_list[17], (2 * SEP_UP, BLOCK), BLOCK ** -0.5, 0.5, ((0, 256),), jnp.float32),
        "expand_upper": centred(key_list[18], (2 * SEP_UP, RANK), RANK ** -0.5, 0.5, ((0, 256),), jnp.float32),
        "basis_upper": centred(key_list[19], (2 * SEP_UP, 2 * RANK), SEP_UP ** -0.5, 0.046875, ((0, 256),), jnp.float32),
        "pivot_upper": jnp.clip(jax.random.uniform(key_list[20], (2 * SEP_UP,), jnp.float32, -2.0, 2.0) * level_of(key_list[20], (2 * SEP_UP,), ((0, 256),), -0.4, 0.0), -2.0, 2.0),
        "couple_upper": centred(key_list[21], (2 * SEP_UP, RANK), RANK ** -0.5, 0.5, ((0, 256),), jnp.float32),
        "ranks_upper": set_ends(jax.random.randint(key_list[22], (2, 2), RANK // 4, RANK + 1), jax.random.fold_in(key_list[22], 1), RANK // 4, RANK).astype(jnp.int32),
        "targets_upper": draw_targets_upper(jax.random.fold_in(key_list[30], 71), 0),
        "source_root": centred(key_list[24], (RHS_COUNT, SEP_ROOT), 1.0, 6.0, ((1, 256),), jnp.float32),
        "block_root": centred(key_list[25], (SEP_ROOT, BLOCK), BLOCK ** -0.5, 0.5, ((0, 256),), jnp.float32),
        "expand_root": centred(key_list[26], (SEP_ROOT, RANK), RANK ** -0.5, 0.5, ((0, 256),), jnp.float32),
        "basis_root": centred(key_list[27], (SEP_ROOT, 2 * RANK), SEP_ROOT ** -0.5, 0.03125, ((0, 256),), jnp.float32),
        "pivot_root": jnp.clip(jax.random.uniform(key_list[28], (SEP_ROOT,), jnp.float32, -2.0, 2.0) * level_of(key_list[28], (SEP_ROOT,), ((0, 256),), -0.4, 0.0), -2.0, 2.0),
        "ranks_root": jax.random.randint(key_list[29], (1, 2), RANK // 4, RANK + 1).astype(jnp.int32),
    }


HIGH_PRECISION = lax.Precision.HIGHEST


def make_masks(ranks):
    cols = jnp.arange(RANK, dtype=jnp.int32)
    head_mask_grid = (cols[None, :] < ranks[:, 0:1]).astype(jnp.float32)[:, None, :]
    column_mask_grid = (cols[None, :] < ranks[:, 1:2]).astype(jnp.float32)[:, None, :]
    return head_mask_grid, column_mask_grid


def forward(source, inc_sep, block, expand, basis, pivot, ranks, fronts):
    width = source.shape[1] // fronts
    level_batch_index = source.reshape(RHS_COUNT, fronts, width).transpose(1, 0, 2)
    if inc_sep is not None:
        level_batch_index = level_batch_index + inc_sep
    tiles = block.reshape(fronts, width // BLOCK, BLOCK, BLOCK)
    local_portion = jnp.einsum("fanh,fnhk->fank", level_batch_index.reshape(fronts, RHS_COUNT, width // BLOCK, BLOCK), tiles, precision=HIGH_PRECISION).reshape(fronts, RHS_COUNT, width)
    gens = basis.reshape(fronts, width, 2 * RANK)
    query_lookup = gens[:, :, :RANK]
    coupling_right_factor = gens[:, :, RANK:]
    spread_across_rows = expand.reshape(fronts, width, RANK)
    head_mask_grid, column_mask_grid = make_masks(ranks)
    hidden_query_rows = jnp.einsum("mle,meq->mlq", level_batch_index, query_lookup, precision=HIGH_PRECISION) * head_mask_grid
    intermediate_entries = local_portion + jnp.einsum("gdk,gtk->gdt", hidden_query_rows, spread_across_rows, precision=HIGH_PRECISION)
    weight_entries = jnp.einsum("mle,meq->mlq", intermediate_entries, coupling_right_factor, precision=HIGH_PRECISION) * column_mask_grid
    correction_entries = intermediate_entries * pivot.reshape(fronts, 1, width)
    return correction_entries, weight_entries, (tiles, query_lookup, coupling_right_factor, spread_across_rows, head_mask_grid, column_mask_grid)


def flat_index(targets, fronts, parents, total):
    count = targets.shape[0] // fronts
    owner = jnp.arange(fronts, dtype=jnp.int32) // (fronts // parents)
    return (owner[:, None] * total + targets.reshape(fronts, count).astype(jnp.int32)).reshape(-1)


def scatter_up(update, targets, fronts, parents, sep_par, upd_par):
    total = sep_par + upd_par
    flat = flat_index(targets, fronts, parents, total)
    values = update.transpose(1, 0, 2).reshape(RHS_COUNT, -1)
    buffer = jnp.zeros((RHS_COUNT, parents * total), jnp.float32).at[:, flat].add(values)
    buffer = buffer.reshape(RHS_COUNT, parents, total).transpose(1, 0, 2)
    return buffer[:, :, :sep_par], buffer[:, :, sep_par:]


def pull_down(front_rows, targets, fronts, parents):
    total = front_rows.shape[2]
    flat = flat_index(targets, fronts, parents, total)
    whole = front_rows.transpose(1, 0, 2).reshape(RHS_COUNT, parents * total)
    values = jnp.take(whole, flat, axis=1)
    return values.reshape(RHS_COUNT, fronts, -1).transpose(1, 0, 2)


def backward(correction_entries, x_upd, couple, parts, fronts):
    tiles, query_lookup, coupling_right_factor, spread_across_rows, head_mask_grid, column_mask_grid = parts
    width = correction_entries.shape[2]
    remainder_rows = correction_entries
    if x_upd is not None:
        couple_u = couple.reshape(fronts, -1, RANK)
        solve_direction = jnp.einsum("fau,fur->far", x_upd, couple_u, precision=HIGH_PRECISION) * column_mask_grid
        remainder_rows = correction_entries - jnp.einsum("gdk,gtk->gdt", solve_direction, coupling_right_factor, precision=HIGH_PRECISION)
    right_projection = jnp.einsum("mle,meq->mlq", remainder_rows, spread_across_rows, precision=HIGH_PRECISION) * head_mask_grid
    local_portion = jnp.einsum("fanh,fnkh->fank", remainder_rows.reshape(fronts, RHS_COUNT, width // BLOCK, BLOCK), tiles, precision=HIGH_PRECISION).reshape(fronts, RHS_COUNT, width)
    return local_portion + jnp.einsum("gdk,gtk->gdt", right_projection, query_lookup, precision=HIGH_PRECISION)


def reference(source_leaf, block_leaf, expand_leaf, basis_leaf, pivot_leaf, couple_leaf, ranks_leaf, targets_leaf,
              source_middle, block_middle, expand_middle, basis_middle, pivot_middle, couple_middle, ranks_middle, targets_middle,
              source_upper, block_upper, expand_upper, basis_upper, pivot_upper, couple_upper, ranks_upper, targets_upper,
              source_root, block_root, expand_root, basis_root, pivot_root, ranks_root):
    levels = [
        (source_leaf, block_leaf, expand_leaf, basis_leaf, pivot_leaf, couple_leaf, ranks_leaf, targets_leaf),
        (source_middle, block_middle, expand_middle, basis_middle, pivot_middle, couple_middle, ranks_middle, targets_middle),
        (source_upper, block_upper, expand_upper, basis_upper, pivot_upper, couple_upper, ranks_upper, targets_upper),
        (source_root, block_root, expand_root, basis_root, pivot_root, None, ranks_root, None),
    ]
    fronts = [N_LEAF, 4, 2, 1]
    inc_sep = None
    inc_upd = None
    saved = []
    for level in range(4):
        source, block, expand, basis, pivot, couple, ranks, targets = levels[level]
        correction_entries, weight_entries, parts = forward(source, inc_sep, block, expand, basis, pivot, ranks, fronts[level])
        saved.append((correction_entries, parts))
        if level < 3:
            couple_u = couple.reshape(fronts[level], -1, RANK)
            update = -jnp.einsum("far,fur->fau", weight_entries, couple_u, precision=HIGH_PRECISION)
            if inc_upd is not None:
                update = update + inc_upd
            sep_par = levels[level + 1][0].shape[1] // fronts[level + 1]
            upd_par = 0
            if level + 1 < 3:
                upd_par = levels[level + 1][5].shape[0] // fronts[level + 1]
            inc_sep, inc_upd = scatter_up(update, targets, fronts[level], fronts[level + 1], sep_par, upd_par)
            if upd_par == 0:
                inc_upd = None
    answers = [None, None, None, None]
    rows_par = None
    for level in (3, 2, 1, 0):
        correction_entries, parts = saved[level]
        couple = levels[level][5]
        targets = levels[level][7]
        x_upd = None
        if level < 3:
            x_upd = pull_down(rows_par, targets, fronts[level], fronts[level + 1])
        xvals = backward(correction_entries, x_upd, couple, parts, fronts[level])
        answers[level] = xvals.transpose(1, 0, 2).reshape(RHS_COUNT, -1)
        rows_par = xvals if x_upd is None else jnp.concatenate([xvals, x_upd], axis=2)
    return (answers[0], answers[1], answers[2], answers[3])
```

```python
import functools

import jax
import jax.numpy as jnp
from jax import lax
from jax.experimental import pallas as pl
from jax.experimental.pallas import tpu as pltpu
from jax.sharding import PartitionSpec as P

RHS = 8
LANES = 128
TILE = 128
SLOT = 32
SLOTS_LEAF = 4

F32 = jnp.float32
HIGHEST = lax.Precision.HIGHEST


def dot(a, b, ca, cb):
    return lax.dot_general(
        a, b, (((ca,), (cb,)), ((), ())), precision=HIGHEST, preferred_element_type=F32
    )


def mm(a, b):
    return dot(a, b, 1, 0)


def mmt(a, b):
    return dot(a, b, 1, 1)


def iota(shape, dim):
    return lax.broadcasted_iota(jnp.int32, shape, dim)


def masks(ranks_ref, groups):
    front = lax.axis_index("leaf") // groups
    pair = ranks_ref[pl.ds(front, 1), :]
    lane = iota((1, TILE), 1)
    mh = (lane < pair[:, 0:1]).astype(F32)
    mc = (lane < pair[:, 1:2]).astype(F32)
    return mh, mc


def spread(parts):
    n = parts[0][0].shape[1]
    rows = []
    for values, label in parts:
        rows.append(values)
        tail = SLOT - RHS
        if label is None:
            rows.append(jnp.zeros((tail, n), F32))
        else:
            at = iota((tail, n), 0)
            rows.append(jnp.where(at == 0, jnp.broadcast_to(label, (tail, n)), 0.0))
    left = LANES - SLOT * len(parts)
    if left:
        rows.append(jnp.zeros((left, n), F32))
    return jnp.concatenate(rows, axis=0)


def dest_onehot(dest, count):
    n = dest.shape[1]
    return (iota((count, n), 0) == jnp.broadcast_to(dest, (count, n))).astype(F32)


def split_target(targets, shift):
    piece = lax.shift_right_logical(targets, shift)
    within = jnp.bitwise_and(targets, (1 << shift) - 1)
    dest = lax.shift_right_logical(within, 7)
    label = piece * TILE + jnp.bitwise_and(within, TILE - 1)
    return dest, label.astype(F32)


def leaf_slots(onehot):
    n = onehot.shape[1]
    upper = (iota((n, n), 0) <= iota((n, n), 1)).astype(F32)
    order = lax.dot_general(
        onehot, upper, (((1,), (0,)), ((), ())), preferred_element_type=F32
    )
    return jnp.sum(order * onehot, axis=0, keepdims=True) - 1.0


def label_onehot(got, k, cols):
    count = got.shape[0]
    label = got[:, SLOT * k + RHS : SLOT * k + RHS + 1]
    at = iota((count, cols), 1).astype(F32)
    return (jnp.broadcast_to(label, (count, cols)) == at).astype(F32)


def received(got, slots, cols):
    turned = got.T
    total = None
    for k in range(slots):
        part = mm(turned[SLOT * k : SLOT * k + RHS, :], label_onehot(got, k, cols))
        total = part if total is None else total + part
    return total


def replies(got, rows, slots):
    total = None
    zero = jnp.zeros_like(rows)
    for k in range(slots):
        padded = spread([(rows if j == k else zero, None) for j in range(slots)])
        part = mmt(label_onehot(got, k, rows.shape[1]), padded)
        total = part if total is None else total + part
    return total


def sum_copies(ref, copies, rows):
    total = ref[0:rows, :]
    for i in range(1, copies):
        total = total + ref[rows * i : rows * (i + 1), :]
    return total


def start_kernel(
    src, w, p, q, tl, pm, qm, pu, qu, pr, pivr, first, y0, slot, cross
):
    b = src[...]
    y = mm(b, w[...])
    v = q[:, RANK_AT:]
    first[0:RHS, :] = mm(b, q[:, 0:RANK_AT])
    first[RHS : 2 * RHS, :] = mm(y, v)
    first[2 * RHS :, :] = dot(p[...], v, 0, 0)
    y0[...] = y
    dest, _ = split_target(tl[...], 13)
    slot[...] = leaf_slots(dest_onehot(dest, 64))
    cross[0:TILE, :] = dot(pm[...], qm[:, RANK_AT:], 0, 0)
    cross[TILE : 2 * TILE, :] = dot(pu[...], qu[:, RANK_AT:], 0, 0)
    scaled = pr[...].T * pivr[...]
    cross[2 * TILE :, :] = mm(scaled, pr[...])


RANK_AT = 128


def leaf_up_kernel(s0, s1, s2, s3, y0, p, piv, c, ranks, tl, slot, out, z_out, zp_out, k_out):
    total = (s0[...] + s1[...]) + (s2[...] + s3[...])
    mh, mc = masks(ranks, 1)
    k1 = total[2 * RHS :, :]
    hq = total[0:RHS, :] * mh
    wv = (total[RHS : 2 * RHS, :] + mm(hq, k1)) * mc
    e = -mmt(wv, c[...])
    dest, label = split_target(tl[...], 13)
    pick = dest_onehot(dest, 64)
    at = slot[...]
    parts = []
    for k in range(SLOTS_LEAF):
        on = (at == float(k)).astype(F32)
        parts.append((e * on, label * on))
    out[...] = mmt(pick, spread(parts))
    z = (y0[...] + mmt(hq, p[...])) * piv[...]
    z_out[...] = z
    zp_out[...] = mm(z, p[...])
    k_out[...] = k1


def enter_kernel(slots, has_update, got, src, w, q, part, y0, upd=None):
    g = got[...]
    cols = 2 * TILE if has_update else TILE
    inc = received(g, slots, cols)
    b = src[...] + inc[:, 0:TILE]
    y = mm(b, w[...])
    part[0:RHS, :] = mm(b, q[:, 0:RANK_AT])
    part[RHS:, :] = mm(y, q[:, RANK_AT:])
    y0[...] = y
    if has_update:
        upd[...] = inc[:, TILE:]


def enter_root_kernel(got, src, w, p, q, piv, part, y0):
    inc = received(got[...], 1, TILE)
    b = src[...] + inc
    y = mm(b, w[...])
    part[0:RHS, :] = mm(b, q[:, 0:RANK_AT])
    part[RHS:, :] = mm(y * piv[...], p[...])
    y0[...] = y


def up_kernel(copies, groups, shift, peers, red, y0, upd, p, piv, c, ranks, t, k1, out, z_out, zp_out):
    total = sum_copies(red, copies, 2 * RHS)
    mh, mc = masks(ranks, groups)
    hq = total[0:RHS, :] * mh
    wv = (total[RHS:, :] + mm(hq, k1[...])) * mc
    e = upd[...] - mmt(wv, c[...])
    dest, label = split_target(t[...], shift)
    out[...] = mmt(dest_onehot(dest, peers), spread([(e, label)]))
    z = (y0[...] + mmt(hq, p[...])) * piv[...]
    z_out[...] = z
    zp_out[...] = mm(z, p[...])


def root_kernel(copies, red, y0, w, p, q, piv, ranks, k2, got, answer, reply):
    total = sum_copies(red, copies, 2 * RHS)
    mh, _ = masks(ranks, 64)
    hq = total[0:RHS, :] * mh
    pr = (total[RHS:, :] + mm(hq, k2[...])) * mh
    r = (y0[...] + mmt(hq, p[...])) * piv[...]
    x = mmt(r, w[...]) + mmt(pr, q[:, 0:RANK_AT])
    answer[...] = x
    reply[...] = replies(got[...], x, 1)


def fetch_kernel(shift, peers, back, t, c, zp, part, xu_out):
    dest, _ = split_target(t[...], shift)
    turned = back[...].T
    xu = mm(turned[0:RHS, :], dest_onehot(dest, peers))
    part[0:RHS, :] = mm(xu, c[...])
    part[RHS:, :] = zp[...]
    xu_out[...] = xu


def fetch_leaf_kernel(back, t, slot, c, zp, part):
    dest, _ = split_target(t[...], 13)
    turned = back[...].T
    rows = jnp.concatenate(
        [turned[SLOT * k : SLOT * k + RHS, :] for k in range(SLOTS_LEAF)], axis=0
    )
    both = mm(rows, dest_onehot(dest, 64))
    at = slot[...]
    xu = None
    for k in range(SLOTS_LEAF):
        one = both[RHS * k : RHS * (k + 1), :] * (at == float(k)).astype(F32)
        xu = one if xu is None else xu + one
    part[0:RHS, :] = mm(xu, c[...])
    part[RHS:, :] = zp[...]


def solve(total, z, k1, w, q, mh, mc):
    s = total[0:RHS, :] * mc
    r = z - mmt(s, q[:, RANK_AT:])
    pr = (total[RHS:, :] - mmt(s, k1)) * mh
    return mmt(r, w) + mmt(pr, q[:, 0:RANK_AT])


def down_kernel(copies, groups, slots, red, z, k1, w, q, ranks, xu, got, answer, reply):
    total = sum_copies(red, copies, 2 * RHS)
    mh, mc = masks(ranks, groups)
    x = solve(total, z[...], k1[...], w[...], q[...], mh, mc)
    answer[...] = x
    reply[...] = replies(got[...], jnp.concatenate([x, xu[...]], axis=1), slots)


def leaf_kernel(s0, s1, s2, s3, z, k1, w, q, ranks, answer):
    total = (s0[...] + s1[...]) + (s2[...] + s3[...])
    mh, mc = masks(ranks, 1)
    answer[...] = solve(total, z[...], k1[...], w[...], q[...], mh, mc)


def run(kernel, shapes, *args):
    outs = [jax.ShapeDtypeStruct(s, F32) for s in shapes]
    name = getattr(kernel, "func", kernel).__name__
    single = len(outs) == 1
    return pl.pallas_call(
        kernel,
        out_shape=outs[0] if single else outs,
        name=name,
    )(*args)


def swap(value, axis, mask):
    pairs = [(s, s ^ mask) for s in range(lax.axis_size(axis))]
    return lax.ppermute(value, axis, pairs)


def four(value, axis, unit):
    return [value] + [swap(value, axis, unit * m) for m in (1, 2, 3)]


def add_four(values):
    return (values[0] + values[1]) + (values[2] + values[3])


def share(value, members):
    rows = value.shape[0]
    copies = jnp.broadcast_to(value, (members, *value.shape)).reshape(members * rows, LANES)
    size = lax.axis_size("leaf")
    groups = None
    if members < size:
        groups = [list(range(g, g + members)) for g in range(0, size, members)]
    return lax.all_to_all(
        copies, "leaf", split_axis=0, concat_axis=0, tiled=True, axis_index_groups=groups
    )


def route(messages, members):
    size = lax.axis_size("leaf") * lax.axis_size("grid")
    groups = None
    if members < size:
        groups = [list(range(g, g + members)) for g in range(0, size, members)]
    return lax.all_to_all(
        messages,
        ("leaf", "grid"),
        split_axis=0,
        concat_axis=0,
        tiled=True,
        axis_index_groups=groups,
    )


def shards(
    src_l, w_l, p_l, q_l, piv_l, c_l, ranks_l, t_l,
    src_m, w_m, p_m, q_m, piv_m, c_m, ranks_m, t_m,
    src_u, w_u, p_u, q_u, piv_u, c_u, ranks_u, t_u,
    src_r, w_r, p_r, q_r, piv_r, ranks_r,
):
    t_l, t_m, t_u = (t.reshape(1, -1) for t in (t_l, t_m, t_u))
    piv_l, piv_m, piv_u, piv_r = (v.reshape(1, -1) for v in (piv_l, piv_m, piv_u, piv_r))
    row = (RHS, TILE)
    pair = (2 * RHS, TILE)

    first, y_l, slot_l, cross = run(
        start_kernel,
        [(2 * RHS + TILE, TILE), row, (1, 2 * TILE), (3 * TILE, TILE)],
        src_l, w_l, p_l, q_l, t_l, p_m, q_m, p_u, q_u, p_r, piv_r,
    )
    for axis, mask in (("grid", 1), ("grid", 2), ("leaf", 1), ("leaf", 2), ("leaf", 4), ("leaf", 8)):
        cross = cross + swap(cross, axis, mask)
    k_m = cross[0:TILE]
    cross = cross[TILE:]
    cross = cross + swap(cross, "leaf", 16)
    k_u = cross[0:TILE]
    k_r = cross[TILE:]
    k_r = k_r + swap(k_r, "leaf", 32)

    out, z_l, zp_l, k_l = run(
        leaf_up_kernel,
        [(64, LANES), row, row, (TILE, TILE)],
        *four(first, "grid", 1), y_l, p_l, piv_l, c_l, ranks_l, t_l, slot_l,
    )
    got_m = route(out, 64)

    part, y_m, upd_m = run(
        functools.partial(enter_kernel, SLOTS_LEAF, True), [pair, row, row],
        got_m, src_m, w_m, q_m,
    )
    red = share(add_four(four(part, "grid", 1)), 16)
    out, z_m, zp_m = run(
        functools.partial(up_kernel, 16, 16, 14, 128), [(128, LANES), row, row],
        red, y_m, upd_m, p_m, piv_m, c_m, ranks_m, t_m, k_m,
    )
    got_u = route(out, 128)

    part, y_u, upd_u = run(
        functools.partial(enter_kernel, 1, True), [pair, row, row],
        got_u, src_u, w_u, q_u,
    )
    red = share(add_four(four(part, "grid", 1)), 32)
    out, z_u, zp_u = run(
        functools.partial(up_kernel, 32, 32, 15, 256), [(256, LANES), row, row],
        red, y_u, upd_u, p_u, piv_u, c_u, ranks_u, t_u, k_u,
    )
    got_r = route(out, 256)

    part, y_r = run(enter_root_kernel, [pair, row], got_r, src_r, w_r, p_r, q_r, piv_r)
    part = add_four(four(part, "grid", 1))
    red = share(add_four(four(part, "leaf", 16)), 16)
    x_r, out = run(
        functools.partial(root_kernel, 16), [row, (256, LANES)],
        red, y_r, w_r, p_r, q_r, piv_r, ranks_r, k_r, got_r,
    )

    back = route(out, 256)
    part, xu = run(
        functools.partial(fetch_kernel, 15, 256), [pair, row], back, t_u, c_u, zp_u
    )
    red = share(add_four(four(part, "grid", 1)), 32)
    x_u, out = run(
        functools.partial(down_kernel, 32, 32, 1), [row, (128, LANES)],
        red, z_u, k_u, w_u, q_u, ranks_u, xu, got_u,
    )

    back = route(out, 128)
    part, xu = run(
        functools.partial(fetch_kernel, 14, 128), [pair, row], back, t_m, c_m, zp_m
    )
    red = share(add_four(four(part, "grid", 1)), 16)
    x_m, out = run(
        functools.partial(down_kernel, 16, 16, SLOTS_LEAF), [row, (64, LANES)],
        red, z_m, k_m, w_m, q_m, ranks_m, xu, got_m,
    )

    back = route(out, 64)
    part = run(fetch_leaf_kernel, [pair], back, t_l, slot_l, c_l, zp_l)
    x_l = run(
        leaf_kernel, [row], *four(part, "grid", 1), z_l, k_l, w_l, q_l, ranks_l
    )
    return (x_l, x_m, x_u, x_r)


def solution(mesh):
    both = ("leaf", "grid")
    wide = P(None, both)
    tall = P(both, None)
    flat = P(both)
    level = (wide, tall, tall, tall, flat, tall, P(), flat)
    in_specs = level * 3 + (wide, tall, tall, tall, flat, P())
    return jax.shard_map(
        shards, mesh=mesh, in_specs=in_specs, out_specs=(wide,) * 4, check_vma=False
    )
```

```python
import functools

import jax
import jax.numpy as jnp
from jax import lax
from jax.experimental import pallas as pl
from jax.experimental.pallas import tpu as pltpu
from jax.sharding import PartitionSpec as P

RHS = 8
LANES = 128
TILE = 128
HOLD = 8
SLOT = 16
SLOTS_LEAF = 4

SRC, WAT, QAT, VAT, MISC, CAT, PAT, END = 0, 8, 136, 264, 392, 400, 528, 656
RMISC, RPAT, REND = 264, 272, 400

F32 = jnp.float32
BF16 = jnp.bfloat16


def iota(shape, dim):
    return lax.broadcasted_iota(jnp.int32, shape, dim)


def raw(a, b, ca, cb):
    return lax.dot_general(a, b, (((ca,), (cb,)), ((), ())), preferred_element_type=F32)


def halves(a):
    high = a.astype(BF16)
    low = (a - high.astype(F32)).astype(BF16)
    return high, low


def stacked(a):
    high = a.astype(BF16).astype(F32)
    return jnp.concatenate([high, a - high], axis=0).astype(BF16)


def fold(total):
    rows = total.shape[0] // 2
    return total[0:rows] + total[rows:]


def dot(a, b, ca, cb):
    high, low = halves(b)
    both = stacked(a)
    return fold(raw(both, high, ca, cb) + raw(both, low, ca, cb))


def mm(a, b):
    return dot(a, b, 1, 0)


def mmt(a, b):
    return dot(a, b, 1, 1)


def cross_product(a, b):
    return lax.dot_general(
        a,
        b,
        (((0,), (0,)), ((), ())),
        precision=lax.Precision.HIGHEST,
        preferred_element_type=F32,
    )


def cross(a, b):
    a_high, a_low = halves(a)
    b_high, b_low = halves(b)
    return (raw(a_low, b_high, 0, 0) + raw(a_high, b_low, 0, 0)) + raw(a_high, b_high, 0, 0)


def masks(ranks_ref, groups):
    front = lax.axis_index("leaf") // groups
    pair = ranks_ref[pl.ds(front, 1), :]
    lane = iota((1, TILE), 1)
    mh = (lane < pair[:, 0:1]).astype(F32)
    mc = (lane < pair[:, 1:2]).astype(F32)
    return mh, mc


def split_target(targets, shift):
    piece = lax.shift_right_logical(targets, shift)
    within = jnp.bitwise_and(targets, (1 << shift) - 1)
    dest = lax.shift_right_logical(within, 7)
    label = piece * TILE + jnp.bitwise_and(within, TILE - 1)
    return dest, label.astype(F32)


def row_onehot(at, count):
    n = at.shape[1]
    if at.dtype == jnp.int32:
        rows = iota((count, n), 0)
    else:
        rows = iota((count, n), 0).astype(F32)
    return (rows == jnp.broadcast_to(at, (count, n))).astype(F32)


def leaf_slots(onehot):
    n = onehot.shape[1]
    upper = (iota((n, n), 0) <= iota((n, n), 1)).astype(BF16)
    order = raw(onehot.astype(BF16), upper, 1, 0)
    return jnp.sum(order * onehot, axis=0, keepdims=True) - 1.0


def label_rows(label):
    n = label.shape[1]
    return jnp.where(iota((SLOT - RHS, n), 0) == 0, jnp.broadcast_to(label, (SLOT - RHS, n)), 0.0)


def fill(rows, n):
    used = sum(r.shape[0] for r in rows)
    if used < LANES:
        rows = rows + [jnp.zeros((LANES - used, n), F32)]
    return jnp.concatenate(rows, axis=0)


def block_mask(n):
    own = jnp.bitwise_and(iota((HOLD * RHS, n), 1), HOLD - 1)
    return (lax.shift_right_logical(iota((HOLD * RHS, n), 0), 3) == own).astype(F32)


def received(turned, slots, cols):
    n = turned.shape[1]
    mask = block_mask(n)
    total = None
    for k in range(slots):
        values = turned[SLOT * k : SLOT * k + RHS, :]
        label = turned[SLOT * k + RHS : SLOT * k + RHS + 1, :]
        spread = jnp.concatenate([values] * HOLD, axis=0) * mask
        part = raw(stacked(spread), row_onehot(label, cols).astype(BF16), 1, 1)
        total = part if total is None else total + part
    return fold(total)


def replies(turned, slots, rows):
    n = turned.shape[1]
    mask = block_mask(n)
    both = stacked(rows)
    out = []
    for k in range(slots):
        label = turned[SLOT * k + RHS : SLOT * k + RHS + 1, :]
        found = fold(raw(both, row_onehot(label, rows.shape[1]).astype(BF16), 1, 0)) * mask
        one = found[0:RHS]
        for j in range(1, HOLD):
            one = one + found[RHS * j : RHS * (j + 1)]
        out += [one, jnp.zeros((SLOT - RHS, n), F32)]
    return fill(out, n).T


def messages(blocks, targets, shift, count):
    out = []
    for b in range(HOLD):
        dest, label = split_target(targets[b : b + 1], shift)
        one = jnp.concatenate([blocks[b], label_rows(label)], axis=0)
        out.append(fold(raw(stacked(one), row_onehot(dest, count).astype(BF16), 1, 1)))
    return fill(out, count).T


def fetched(back, targets, shift):
    turned = back.T
    count = turned.shape[1]
    out = []
    for b in range(HOLD):
        dest, _ = split_target(targets[b : b + 1], shift)
        values = turned[SLOT * b : SLOT * b + RHS, :]
        out.append(fold(raw(stacked(values), row_onehot(dest, count).astype(BF16), 1, 0)))
    return out


def lanes(blocks):
    return jnp.concatenate(blocks, axis=1)


def tall(blocks):
    return jnp.concatenate(blocks, axis=0)


def cut_lanes(value):
    return [value[:, TILE * b : TILE * (b + 1)] for b in range(HOLD)]


def cut_tall(value):
    return [value[RHS * b : RHS * (b + 1)] for b in range(HOLD)]


def own_number():
    core = jnp.bitwise_and(lax.axis_index("leaf"), 1)
    return core * 4 + lax.axis_index("grid")


def numbers():
    core = jnp.bitwise_and(lax.axis_index("leaf"), 1)
    at = lax.axis_index("grid")
    out = []
    for c in (core, 1 - core):
        for step in (0, 3, 1, 2):
            out.append(c * 4 + jnp.bitwise_and(at + step, 3))
    return out


class Held:
    def __init__(self, bufs, base, low, high, scratch, sems):
        self.low = low
        self.scratch = scratch
        self.copies = []
        for i, (buf, at) in enumerate(zip(bufs, numbers())):
            copy = pltpu.make_async_copy(
                buf.at[pl.ds(base + low, high - low)], scratch.at[at], sems.at[i]
            )
            copy.start()
            self.copies.append(copy)

    def wait(self):
        for copy in self.copies:
            copy.wait()

    def one(self, b, at, rows=TILE):
        return self.scratch[b, at - self.low : at - self.low + rows, :]

    def all(self, at):
        return self.scratch[:, at - self.low : at - self.low + TILE, :].reshape(
            HOLD * TILE, TILE
        )

    def misc(self, at, row):
        return jnp.concatenate([self.one(b, at + row, 1) for b in range(HOLD)], axis=0)


def by_tiles(blocks, held, at, turned=False):
    return [
        dot(blocks[b], held.one(b, at), 1, 1 if turned else 0) for b in range(HOLD)
    ]


def split_refs(refs, n_in, n_out):
    bufs = refs[0:HOLD]
    ins = refs[HOLD : HOLD + n_in]
    outs = refs[HOLD + n_in : HOLD + n_in + n_out]
    scratch, sems = refs[HOLD + n_in + n_out :]
    return bufs, ins, outs, scratch, sems


def leaf_start_kernel(src, w, p, q, tl, first, y0, slot):
    b = src[...]
    y = mm(b, w[...])
    v = q[:, TILE:]
    first[0:RHS, :] = mm(b, q[:, 0:TILE])
    first[RHS : 2 * RHS, :] = mm(y, v)
    first[2 * RHS :, :] = cross_product(p[...], v)
    y0[...] = y
    dest, _ = split_target(tl[...], 13)
    slot[...] = leaf_slots(row_onehot(dest, 64))


def pack_kernel(*refs):
    (sm, wm, pm, qm, vm, cm, tm), rest = refs[0:7], refs[7:]
    (su, wu, pu, qu, vu, cu, tu), rest = rest[0:7], rest[7:]
    (sr, wr, pr, qr, vr), rest = rest[0:5], rest[5:]
    pack_m, pack_u = rest
    for pack, s, wt, pt, qt, vt, ct, t in (
        (pack_m, sm, wm, pm, qm, vm, cm, tm),
        (pack_u, su, wu, pu, qu, vu, cu, tu),
    ):
        pack[SRC:WAT, :] = s[...]
        pack[WAT:QAT, :] = wt[...]
        pack[QAT:VAT, :] = qt[:, 0:TILE]
        pack[VAT:MISC, :] = qt[:, TILE:]
        at = iota((8, TILE), 0)
        pack[MISC:CAT, :] = jnp.where(
            at == 0,
            jnp.broadcast_to(vt[...], (8, TILE)),
            jnp.broadcast_to(t[...].astype(F32), (8, TILE)),
        )
        pack[CAT:PAT, :] = ct[...]
        pack[PAT:END, :] = pt[...]
    pack_u[END + SRC : END + WAT, :] = sr[...]
    pack_u[END + WAT : END + QAT, :] = wr[...]
    pack_u[END + QAT : END + RMISC, :] = qr[:, 0:TILE]
    pack_u[END + RMISC : END + RPAT, :] = jnp.broadcast_to(vr[...], (8, TILE))
    pack_u[END + RPAT : END + REND, :] = pr[...]


def cross_kernel(*refs):
    bufs, (), (k1, k2), scratch, sems = split_refs(refs, 0, 2)
    upper = Held(bufs, 0, VAT, END, scratch.at[:, 0 : END - VAT, :], sems.at[0])
    root = Held(bufs, END, RMISC, REND, scratch.at[:, END - VAT :, :], sems.at[1])
    upper.wait()
    k1[...] = cross(upper.all(PAT), upper.all(VAT))
    root.wait()
    total = None
    for b in range(HOLD):
        p = root.one(b, RPAT)
        part = mm(p.T * root.one(b, RMISC, 1), p)
        total = part if total is None else total + part
    k2[...] = total


def leaf_up_kernel(
    s0, s1, s2, s3, y0, p, piv, c, ranks, tl, slot, out, z_out, zp_out, k_out
):
    total = (s0[...] + s1[...]) + (s2[...] + s3[...])
    mh, mc = masks(ranks, 1)
    k1 = total[2 * RHS :, :]
    hq = total[0:RHS, :] * mh
    wv = (total[RHS : 2 * RHS, :] + mm(hq, k1)) * mc
    e = -mmt(wv, c[...])
    dest, label = split_target(tl[...], 13)
    both = jnp.concatenate([e, label_rows(label)], axis=0)
    at = slot[...]
    parts = jnp.concatenate(
        [both * (at == float(k)).astype(F32) for k in range(SLOTS_LEAF)], axis=0
    )
    sent = fold(raw(stacked(parts), row_onehot(dest, 64).astype(BF16), 1, 1))
    sent = fill([sent], 64).T
    for place in range(HOLD):
        part = sent[HOLD * place : HOLD * (place + 1), :]
        for copy in range(HOLD):
            low = (place * HOLD + copy) * HOLD
            out[low : low + HOLD, :] = part
    z = (y0[...] + mmt(hq, p[...])) * piv[...]
    z_out[...] = z
    zp_out[...] = mm(z, p[...])
    k_out[...] = k1


def write_copies(ref, value):
    rows = value.shape[0]
    for i in range(ref.shape[0] // rows):
        ref[rows * i : rows * (i + 1), :] = value


def write_shares(ref, members, value, parts):
    step = ref.shape[0] // members
    rows = step - parts.shape[0] // min(members, 16)
    each = step - rows
    common = value.shape[0] == rows
    for i in range(members):
        low = step * i
        ref[low : low + rows, :] = value if common else value[rows * i : rows * (i + 1)]
        at = each * (i % 16)
        ref[low + rows : low + step, :] = parts[at : at + each]


def sum_rows(ref, step, low, high):
    total = ref[low:high, :]
    for i in range(1, ref.shape[0] // step):
        total = total + ref[step * i + low : step * i + high, :]
    return total


def stack_rows(ref, step, low, high, count):
    return jnp.concatenate(
        [ref[step * i + low : step * i + high, :] for i in range(count)], axis=0
    )


def enter_middle_kernel(*refs):
    bufs, (got,), (part, y_out, upd_out), scratch, sems = split_refs(refs, 1, 3)
    held = Held(bufs, 0, SRC, VAT, scratch, sems)
    inc = received(got[...].T, SLOTS_LEAF, 2 * TILE)
    held.wait()
    b = [held.one(j, SRC, RHS) + inc[RHS * j : RHS * (j + 1), 0:TILE] for j in range(HOLD)]
    write_copies(part, mm(lanes(b), held.all(QAT)))
    y_out[...] = lanes(by_tiles(b, held, WAT))
    upd_out[...] = inc[:, TILE:]


def middle_kernel(*refs):
    bufs, (red, y0, ranks), (part, z_out, zp_out), scratch, sems = split_refs(refs, 3, 3)
    held = Held(bufs, 0, VAT, END, scratch, sems)
    mh, _ = masks(ranks, 16)
    hq = sum_rows(red, RHS, 0, RHS) * mh
    held.wait()
    p, v = held.all(PAT), held.all(VAT)
    y = y0[...] + mmt(hq, p)
    write_shares(part, 8, mm(y, v), cross(p, v))
    z = y * lanes([held.one(b, MISC, 1) for b in range(HOLD)])
    z_out[...] = z
    zp_out[...] = mm(z, p)


def middle_up_kernel(*refs):
    bufs, (red, upd, ranks, k1), (out, k_out), scratch, sems = split_refs(refs, 4, 2)
    held = Held(bufs, 0, MISC, PAT, scratch, sems)
    _, mc = masks(ranks, 16)
    total = sum_rows(red, 3 * RHS, 0, 3 * RHS)
    k_out[...] = total[RHS:, :]
    wv = total[0:RHS, :] * mc
    held.wait()
    e = cut_lanes(mmt(wv, held.all(CAT)))
    upds = cut_tall(upd[...])
    targets = held.misc(MISC, 1).astype(jnp.int32)
    sent = messages([u - v for u, v in zip(upds, e)], targets, 14, 128)
    write_shares(out, 16, sent, k1[...])


def enter_upper_kernel(*refs):
    bufs, (got,), (part, y_out, upd_out), scratch, sems = split_refs(refs, 1, 3)
    held = Held(bufs, 0, SRC, MISC, scratch, sems)
    k1 = sum_rows(got, 2 * RHS, RHS, 2 * RHS)
    inc = received(stack_rows(got, 2 * RHS, 0, RHS, 16).T, HOLD, 2 * TILE)
    held.wait()
    b = [held.one(j, SRC, RHS) + inc[RHS * j : RHS * (j + 1), 0:TILE] for j in range(HOLD)]
    y = lanes(by_tiles(b, held, WAT))
    write_copies(part, tall([mm(lanes(b), held.all(QAT)), mm(y, held.all(VAT)), k1]))
    y_out[...] = y
    upd_out[...] = inc[:, TILE:]


def upper_up_kernel(*refs):
    bufs, ins, outs, scratch, sems = split_refs(refs, 5, 4)
    red, y0, upd, ranks, k2 = ins
    out, z_out, zp_out, k_out = outs
    held = Held(bufs, 0, MISC, END, scratch, sems)
    total = sum_rows(red, 3 * RHS, 0, 2 * RHS)
    k1 = stack_rows(red, 3 * RHS, 2 * RHS, 3 * RHS, 16)
    k_out[...] = k1
    mh, mc = masks(ranks, 32)
    hq = total[0:RHS, :] * mh
    wv = (total[RHS:, :] + mm(hq, k1)) * mc
    held.wait()
    e = cut_lanes(mmt(wv, held.all(CAT)))
    upds = cut_tall(upd[...])
    targets = held.misc(MISC, 1).astype(jnp.int32)
    sent = messages([u - v for u, v in zip(upds, e)], targets, 15, 256)
    write_shares(out, 32, sent, k2[...])
    y = y0[...] + mmt(hq, held.all(PAT))
    z = y * lanes([held.one(b, MISC, 1) for b in range(HOLD)])
    z_out[...] = z
    zp_out[...] = mm(z, held.all(PAT))


def enter_root_kernel(*refs):
    bufs, (got,), (part, y_out), scratch, sems = split_refs(refs, 1, 2)
    held = Held(bufs, END, SRC, REND, scratch, sems)
    k2 = sum_rows(got, 2 * RHS, RHS, 2 * RHS)
    inc = received(stack_rows(got, 2 * RHS, 0, RHS, 32).T, HOLD, TILE)
    held.wait()
    b = [held.one(j, SRC, RHS) + inc[RHS * j : RHS * (j + 1)] for j in range(HOLD)]
    y = lanes(by_tiles(b, held, WAT))
    z = y * lanes([held.one(j, RMISC, 1) for j in range(HOLD)])
    write_copies(part, tall([mm(lanes(b), held.all(QAT)), mm(z, held.all(RPAT)), k2]))
    y_out[...] = y


def own_block(blocks):
    me = own_number()
    out = blocks[0]
    for b in range(1, HOLD):
        out = jnp.where(me == b, blocks[b], out)
    return out


def root_kernel(*refs):
    bufs, (red, y0, ranks, got), (answer, reply), scratch, sems = split_refs(refs, 4, 2)
    held = Held(bufs, END, WAT, REND, scratch, sems)
    total = sum_rows(red, 3 * RHS, 0, 2 * RHS)
    k2 = stack_rows(red, 3 * RHS, 2 * RHS, 3 * RHS, 16)
    mh, _ = masks(ranks, 64)
    hq = total[0:RHS, :] * mh
    pr = (total[RHS:, :] + mm(hq, k2)) * mh
    turned = stack_rows(got, 2 * RHS, 0, RHS, 32).T
    held.wait()
    r = y0[...] + mmt(hq, held.all(RPAT))
    r = r * lanes([held.one(j, RMISC, 1) for j in range(HOLD)])
    x = by_tiles(cut_lanes(r), held, WAT, True)
    low = cut_lanes(mmt(pr, held.all(QAT)))
    x = [u + v for u, v in zip(x, low)]
    answer[...] = own_block(x)
    reply[...] = replies(turned, HOLD, tall(x))


def fetch_kernel(shift, with_cross, *refs):
    n_in = 3 if with_cross else 2
    bufs, ins, (part, xu_out), scratch, sems = split_refs(refs, n_in, 2)
    back, zp = ins[0:2]
    held = Held(bufs, 0, MISC, PAT, scratch, sems)
    held.wait()
    targets = held.misc(MISC, 1).astype(jnp.int32)
    xu = fetched(back[...], targets, shift)
    write_copies(
        part, tall([mm(lanes(xu), held.all(CAT))] + [ref[...] for ref in ins[1:]])
    )
    xu_out[...] = tall(xu)


def solve_held(total, z, k1, held, mh, mc):
    s = total[0:RHS, :] * mc
    r = z - mmt(s, held.all(VAT))
    pr = (total[RHS:, :] - mmt(s, k1)) * mh
    x = by_tiles(cut_lanes(r), held, WAT, True)
    low = cut_lanes(mmt(pr, held.all(QAT)))
    return [u + v for u, v in zip(x, low)]


def down_kernel(groups, *refs):
    middle = groups == 16
    n_in = 5 if middle else 6
    bufs, ins, (answer, reply), scratch, sems = split_refs(refs, n_in, 2)
    red, z, ranks, xu, got = ins[0:5]
    held = Held(bufs, 0, WAT, MISC, scratch, sems)
    mh, mc = masks(ranks, groups)
    if middle:
        total = sum_rows(red, 4 * RHS, 0, 2 * RHS)
        k1 = stack_rows(red, 4 * RHS, 2 * RHS, 4 * RHS, 8)
        me = own_number()
        rows = [
            got[pl.ds(pl.multiple_of((HOLD * i + me) * HOLD, HOLD), HOLD), :]
            for i in range(HOLD)
        ]
        turned, slots = tall(rows).T, SLOTS_LEAF
    else:
        total = sum_rows(red, 2 * RHS, 0, 2 * RHS)
        k1 = ins[5][...]
        turned, slots = stack_rows(got, 2 * RHS, 0, RHS, 16).T, HOLD
    held.wait()
    x = solve_held(total, z[...], k1, held, mh, mc)
    answer[...] = own_block(x)
    reply[...] = replies(turned, slots, jnp.concatenate([tall(x), xu[...]], axis=1))


def fetch_leaf_kernel(back, t, slot, c, zp, part):
    dest, _ = split_target(t[...], 13)
    turned = back[...].T
    rows = tall([turned[SLOT * k : SLOT * k + RHS, :] for k in range(SLOTS_LEAF)])
    both = fold(raw(stacked(rows), row_onehot(dest, 64).astype(BF16), 1, 0))
    at = slot[...]
    xu = None
    for k in range(SLOTS_LEAF):
        one = both[RHS * k : RHS * (k + 1), :] * (at == float(k)).astype(F32)
        xu = one if xu is None else xu + one
    part[0:RHS, :] = mm(xu, c[...])
    part[RHS:, :] = zp[...]


def leaf_kernel(s0, s1, s2, s3, z, k1, w, q, ranks, answer):
    total = (s0[...] + s1[...]) + (s2[...] + s3[...])
    mh, mc = masks(ranks, 1)
    s = total[0:RHS, :] * mc
    r = z[...] - mmt(s, q[:, TILE:])
    pr = (total[RHS:, :] - mmt(s, k1[...])) * mh
    answer[...] = mmt(r, w[...]) + mmt(pr, q[:, 0:TILE])


def run(kernel, shapes, *args, held=None, rows=0, twice=False):
    outs = [jax.ShapeDtypeStruct(s, F32) for s in shapes]
    name = getattr(kernel, "func", kernel).__name__
    options = {}
    if held is not None:
        args = tuple(held) + args
        space = pl.BlockSpec(memory_space=pl.ANY)
        options["in_specs"] = [space] * HOLD + [
            pl.BlockSpec(memory_space=pltpu.VMEM) for _ in args[HOLD:]
        ]
        options["scratch_shapes"] = [
            pltpu.VMEM((HOLD, rows, TILE), F32),
            pltpu.SemaphoreType.DMA((2, HOLD) if twice else (HOLD,)),
        ]
    single = len(outs) == 1
    return pl.pallas_call(
        kernel, out_shape=outs[0] if single else outs, name=name, **options
    )(*args)


def swap(value, axis, mask):
    pairs = [(s, s ^ mask) for s in range(lax.axis_size(axis))]
    return lax.ppermute(value, axis, pairs)


def shift(value, step):
    size = lax.axis_size("grid")
    return lax.ppermute(value, "grid", [(s, (s + step) % size) for s in range(size)])


def four(value, axis, unit):
    return [value] + [swap(value, axis, unit * m) for m in (1, 2, 3)]


def add_four(values):
    return (values[0] + values[1]) + (values[2] + values[3])


def together(*values):
    return lax.optimization_barrier(values)


def between(value, members):
    size = lax.axis_size("leaf")
    groups = [
        [start + core + 2 * i for i in range(members)]
        for start in range(0, size, 2 * members)
        for core in range(2)
    ]
    return lax.all_to_all(
        value, "leaf", split_axis=0, concat_axis=0, tiled=True, axis_index_groups=groups
    )


def route_leaf(value):
    size = lax.axis_size("leaf") * lax.axis_size("grid")
    groups = [list(range(g, g + 64)) for g in range(0, size, 64)]
    return lax.all_to_all(
        value,
        ("leaf", "grid"),
        split_axis=0,
        concat_axis=0,
        tiled=True,
        axis_index_groups=groups,
    )


def shards(
    src_l, w_l, p_l, q_l, piv_l, c_l, ranks_l, t_l,
    src_m, w_m, p_m, q_m, piv_m, c_m, ranks_m, t_m,
    src_u, w_u, p_u, q_u, piv_u, c_u, ranks_u, t_u,
    src_r, w_r, p_r, q_r, piv_r, ranks_r,
):
    t_l, t_m, t_u = (t.reshape(1, -1) for t in (t_l, t_m, t_u))
    piv_l, piv_m, piv_u, piv_r = (v.reshape(1, -1) for v in (piv_l, piv_m, piv_u, piv_r))
    row = (RHS, TILE)
    pair = (2 * RHS, TILE)
    flat = (RHS, HOLD * TILE)
    high = (HOLD * RHS, TILE)

    first, y_l, slot_l = run(
        leaf_start_kernel, [(2 * RHS + TILE, TILE), row, (1, 2 * TILE)],
        src_l, w_l, p_l, q_l, t_l,
    )
    sums = four(first, "grid", 1)
    pack_m, pack_u = run(
        pack_kernel, [(END, TILE), (END + REND, TILE)],
        src_m, w_m, p_m, q_m, piv_m, c_m, t_m,
        src_u, w_u, p_u, q_u, piv_u, c_u, t_u,
        src_r, w_r, p_r, q_r, piv_r,
    )
    m_core, u_core = swap(pack_m, "leaf", 1), swap(pack_u, "leaf", 1)
    *sums, pack_m = together(*sums, pack_m)
    m_prev, m_next = shift(pack_m, 1), shift(pack_m, -1)
    out, z_l, zp_l, k_l = run(
        leaf_up_kernel,
        [(64 * HOLD, LANES), row, row, (TILE, TILE)],
        *sums, y_l, p_l, piv_l, c_l, ranks_l, t_l, slot_l,
    )
    got_m = route_leaf(out)
    m_prev, m_next, pack_u = together(m_prev, m_next, pack_u)
    m_opp = jnp.concatenate([shift(m_prev[:MISC], 1), shift(m_next[MISC:], -1)], axis=0)
    m_prev_core, m_next_core = swap(m_prev, "leaf", 1), swap(m_next, "leaf", 1)
    u_prev, u_next = shift(pack_u, 1), shift(pack_u, -1)
    m_opp_core = swap(m_opp, "leaf", 1)
    held_m = (
        pack_m, m_prev, m_next, m_opp, m_core, m_prev_core, m_next_core, m_opp_core,
    )

    part, y_m, upd_m = run(
        enter_middle_kernel, [(8 * RHS, TILE), flat, high], got_m, held=held_m, rows=VAT - SRC
    )
    part, u_prev, u_next = together(part, u_prev, u_next)
    u_opp = jnp.concatenate([shift(u_prev[:END], 1), shift(u_next[END:], -1)], axis=0)
    u_prev_core, u_next_core = swap(u_prev, "leaf", 1), swap(u_next, "leaf", 1)
    red = between(part, 8)
    part, z_m, zp_m = run(
        middle_kernel, [(8 * 3 * RHS, TILE), flat, row],
        red, y_m, ranks_m, held=held_m, rows=END - VAT,
    )
    part, u_opp = together(part, u_opp)
    u_opp_core = swap(u_opp, "leaf", 1)
    held_u = (
        pack_u, u_prev, u_next, u_opp, u_core, u_prev_core, u_next_core, u_opp_core,
    )
    k_u, k_r = run(
        cross_kernel, [(TILE, TILE)] * 2, held=held_u, rows=END - VAT + REND - RMISC,
        twice=True,
    )
    red = between(part, 8)
    out, k_m = run(
        middle_up_kernel, [(16 * 2 * RHS, LANES), pair],
        red, upd_m, ranks_m, k_u, held=held_m, rows=PAT - MISC,
    )
    got_u = between(out, 16)

    part, y_u, upd_u = run(
        enter_upper_kernel, [(16 * 3 * RHS, TILE), flat, high],
        got_u, held=held_u, rows=MISC - SRC,
    )
    red = between(part, 16)
    out, z_u, zp_u, k_u = run(
        upper_up_kernel, [(32 * 2 * RHS, LANES), flat, row, (TILE, TILE)],
        red, y_u, upd_u, ranks_u, k_r, held=held_u, rows=END - MISC,
    )
    got_r = between(out, 32)

    part, y_r = run(
        enter_root_kernel, [(32 * 3 * RHS, TILE), flat],
        got_r, held=held_u, rows=REND - SRC,
    )
    red = between(part, 32)
    x_r, out = run(
        root_kernel, [row, (256, LANES)],
        red, y_r, ranks_r, got_r, held=held_u, rows=REND - WAT,
    )

    back = between(out, 32)
    part, xu = run(
        functools.partial(fetch_kernel, 15, False), [(16 * 2 * RHS, TILE), high],
        back, zp_u, held=held_u, rows=PAT - MISC,
    )
    red = between(part, 16)
    x_u, out = run(
        functools.partial(down_kernel, 32), [row, (128, LANES)],
        red, z_u, ranks_u, xu, got_u, k_u, held=held_u, rows=MISC - WAT,
    )

    back = between(out, 16)
    part, xu = run(
        functools.partial(fetch_kernel, 14, True), [(8 * 4 * RHS, TILE), high],
        back, zp_m, k_m, held=held_m, rows=PAT - MISC,
    )
    red = between(part, 8)
    x_m, out = run(
        functools.partial(down_kernel, 16), [row, (64, LANES)],
        red, z_m, ranks_m, xu, got_m, held=held_m, rows=MISC - WAT,
    )

    back = between(out, 8)
    part = run(fetch_leaf_kernel, [pair], back, t_l, slot_l, c_l, zp_l)
    x_l = run(
        leaf_kernel, [row], *four(part, "grid", 1), z_l, k_l, w_l, q_l, ranks_l
    )
    return (x_l, x_m, x_u, x_r)


def solution(mesh):
    both = ("leaf", "grid")
    wide = P(None, both)
    deep = P(both, None)
    line = P(both)
    level = (wide, deep, deep, deep, line, deep, P(), line)
    in_specs = level * 3 + (wide, deep, deep, deep, line, P())
    return jax.shard_map(
        shards, mesh=mesh, in_specs=in_specs, out_specs=(wide,) * 4, check_vma=False
    )
```

```python
import functools

import jax
import jax.numpy as jnp
from jax import lax
from jax.experimental import pallas as pl
from jax.experimental.pallas import tpu as pltpu
from jax.sharding import PartitionSpec as P

RHS = 8
LANES = 128
TILE = 128
HOLD = 8
SLOT = 16
SLOTS_LEAF = 4

SRC, WAT, QAT, VAT, MISC, CAT, PAT, END = 0, 8, 136, 264, 392, 400, 528, 656
RMISC, RPAT, REND = 264, 272, 400

F32 = jnp.float32
BF16 = jnp.bfloat16


def iota(shape, dim):
    return lax.broadcasted_iota(jnp.int32, shape, dim)


def raw(a, b, ca, cb):
    return lax.dot_general(a, b, (((ca,), (cb,)), ((), ())), preferred_element_type=F32)


def halves(a):
    high = a.astype(BF16)
    low = (a - high.astype(F32)).astype(BF16)
    return high, low


def stacked(a):
    high = a.astype(BF16).astype(F32)
    return jnp.concatenate([high, a - high], axis=0).astype(BF16)


def fold(total):
    rows = total.shape[0] // 2
    return total[0:rows] + total[rows:]


def dot(a, b, ca, cb):
    high, low = halves(b)
    both = stacked(a)
    return fold(raw(both, high, ca, cb) + raw(both, low, ca, cb))


def mm(a, b):
    return dot(a, b, 1, 0)


def mmt(a, b):
    return dot(a, b, 1, 1)


def cross(a, b):
    a_high, a_low = halves(a)
    b_high, b_low = halves(b)
    return (raw(a_low, b_high, 0, 0) + raw(a_high, b_low, 0, 0)) + raw(a_high, b_high, 0, 0)


def mask_rows(ranks_ref, groups):
    front = lax.axis_index("leaf") // groups
    both = ranks_ref[...].astype(F32)
    own = iota(both.shape, 1) == front
    pair = jnp.sum(jnp.where(own, both, 0.0), axis=1, keepdims=True)
    lane = iota((1, TILE), 1).astype(F32)
    return [(lane < pair[i : i + 1, :]).astype(F32) for i in range(2)]


def masks(rows_ref, level):
    return rows_ref[2 * level : 2 * level + 1, :], rows_ref[2 * level + 1 : 2 * level + 2, :]


def split_target(targets, shift):
    piece = lax.shift_right_logical(targets, shift)
    within = jnp.bitwise_and(targets, (1 << shift) - 1)
    dest = lax.shift_right_logical(within, 7)
    label = piece * TILE + jnp.bitwise_and(within, TILE - 1)
    return dest, label.astype(F32)


def row_onehot(at, count):
    n = at.shape[1]
    if at.dtype == jnp.int32:
        rows = iota((count, n), 0)
    else:
        rows = iota((count, n), 0).astype(F32)
    return (rows == jnp.broadcast_to(at, (count, n))).astype(F32)


def leaf_slots(onehot):
    n = onehot.shape[1]
    upper = (iota((n, n), 0) <= iota((n, n), 1)).astype(BF16)
    order = raw(onehot.astype(BF16), upper, 1, 0)
    return jnp.sum(order * onehot, axis=0, keepdims=True) - 1.0


def label_rows(label):
    n = label.shape[1]
    return jnp.where(iota((SLOT - RHS, n), 0) == 0, jnp.broadcast_to(label, (SLOT - RHS, n)), 0.0)


def fill(rows, n):
    used = sum(r.shape[0] for r in rows)
    if used < LANES:
        rows = rows + [jnp.zeros((LANES - used, n), F32)]
    return jnp.concatenate(rows, axis=0)


def block_mask(n):
    lane = jnp.bitwise_and(iota((RHS, n), 1), HOLD - 1)
    return jnp.concatenate([(lane == at).astype(F32) for at in numbers()], axis=0)


def received(turned, slots, cols):
    n = turned.shape[1]
    mask = block_mask(n)
    total = None
    for k in range(slots):
        values = turned[SLOT * k : SLOT * k + RHS, :]
        label = turned[SLOT * k + RHS : SLOT * k + RHS + 1, :]
        spread = jnp.concatenate([values] * HOLD, axis=0) * mask
        part = raw(stacked(spread), row_onehot(label, cols).astype(BF16), 1, 1)
        total = part if total is None else total + part
    return fold(total)


def replies(turned, slots, rows):
    n = turned.shape[1]
    mask = block_mask(n)
    both = stacked(rows)
    out = []
    for k in range(slots):
        label = turned[SLOT * k + RHS : SLOT * k + RHS + 1, :]
        found = fold(raw(both, row_onehot(label, rows.shape[1]).astype(BF16), 1, 0)) * mask
        one = found[0:RHS]
        for j in range(1, HOLD):
            one = one + found[RHS * j : RHS * (j + 1)]
        out += [one, jnp.zeros((SLOT - RHS, n), F32)]
    return fill(out, n).T


def slot_rows(at):
    return pl.ds(pl.multiple_of(SLOT * at, SLOT), SLOT)


def messages(blocks, targets, shift, count, scratch):
    for r, at in enumerate(numbers()):
        dest, label = split_target(targets[r : r + 1], shift)
        one = jnp.concatenate([blocks[r], label_rows(label)], axis=0)
        found = fold(raw(stacked(one), row_onehot(dest, count).astype(BF16), 1, 1))
        scratch[slot_rows(at), :] = found
    return scratch[...].T


def fetched(back, targets, shift, scratch):
    scratch[...] = back.T
    count = scratch.shape[1]
    out = []
    for r, at in enumerate(numbers()):
        dest, _ = split_target(targets[r : r + 1], shift)
        values = scratch[slot_rows(at), :][0:RHS]
        out.append(fold(raw(stacked(values), row_onehot(dest, count).astype(BF16), 1, 0)))
    return out


def lanes(blocks):
    return jnp.concatenate(blocks, axis=1)


def tall(blocks):
    return jnp.concatenate(blocks, axis=0)


def cut_lanes(value):
    return [value[:, TILE * b : TILE * (b + 1)] for b in range(HOLD)]


def cut_tall(value):
    return [value[RHS * b : RHS * (b + 1)] for b in range(HOLD)]


def own_number():
    core = jnp.bitwise_and(lax.axis_index("leaf"), 1)
    return core * 4 + lax.axis_index("grid")


def numbers():
    core = jnp.bitwise_and(lax.axis_index("leaf"), 1)
    at = lax.axis_index("grid")
    out = []
    for c in (core, 1 - core):
        for step in (0, 3, 1, 2):
            out.append(c * 4 + jnp.bitwise_and(at + step, 3))
    return out


class Held:
    def __init__(self, refs, cut, base=0):
        own, prev, after, low, high = refs[0:5]
        self.own = (own, prev, after)
        self.opposite = (low, high)
        self.core = refs[5:8]
        self.core_opposite = refs[8:10]
        self.cut = cut
        self.base = base

    def one(self, b, at, rows=TILE):
        at = at + self.base
        singles, split = (
            (self.own, self.opposite) if b < 4 else (self.core, self.core_opposite)
        )
        if b % 4 < 3:
            ref = singles[b % 4]
        elif at < self.cut:
            ref = split[0]
        else:
            ref = split[1]
            at = at - self.cut
        return ref[at : at + rows, :]

    def all(self, at):
        return jnp.concatenate([self.one(b, at) for b in range(HOLD)], axis=0)

    def misc(self, at, row):
        return jnp.concatenate([self.one(b, at + row, 1) for b in range(HOLD)], axis=0)


class Fetched(Held):
    def __init__(self, refs, cut, low, high, scratch, sems):
        self.low = low
        self.scratch = scratch
        self.copies = []
        own, core = refs[0:5], refs[5:10]
        for half, bufs in enumerate((own, core)):
            for b in range(3):
                self.start(bufs[b], low, low, high, 4 * half + b, sems)
            if low < cut:
                self.start(bufs[3], low, low, min(high, cut), 4 * half + 3, sems)
            if high > cut:
                at = max(low, cut)
                self.start(bufs[4], at - cut, at, high, 4 * half + 3, sems)

    def start(self, buf, source, low, high, b, sems):
        copy = pltpu.make_async_copy(
            buf.at[pl.ds(source, high - low)],
            self.scratch.at[b, pl.ds(low - self.low, high - low)],
            sems.at[len(self.copies)],
        )
        copy.start()
        self.copies.append(copy)

    def wait(self):
        for copy in self.copies:
            copy.wait()

    def one(self, b, at, rows=TILE):
        return self.scratch[b, at - self.low : at - self.low + rows, :]


def by_tiles(blocks, held, at, turned=False):
    return [
        dot(blocks[b], held.one(b, at), 1, 1 if turned else 0) for b in range(HOLD)
    ]


HELD_REFS = 10


LW, LQ, LV, LP, LC, LEND = 0, 128, 256, 384, 512, 768


def leaf_start_kernel(
    src, w, p, q, c, piv, tl, ranks_l, ranks_m, ranks_u, ranks_r,
    first, y0, plan, rows, hold,
):
    b = src[...]
    y = mm(b, w[...])
    v = q[:, TILE:]
    first[0:RHS, :] = mm(b, q[:, 0:TILE])
    first[RHS : 2 * RHS, :] = mm(y, v)
    first[2 * RHS :, :] = cross(p[...], v)
    y0[...] = y
    dest, label = split_target(tl[...], 13)
    plan[0:1, :] = dest.astype(F32)
    plan[1:2, :] = label
    plan[2:3, :] = leaf_slots(row_onehot(dest, 64))
    plan[3:8, :] = jnp.zeros((5, 2 * TILE), F32)
    found = []
    for ranks, groups in ((ranks_l, 1), (ranks_m, 16), (ranks_u, 32), (ranks_r, 64)):
        found += mask_rows(ranks, groups)
    rows[...] = jnp.concatenate(found[0:7] + [piv[...]], axis=0)
    hold[LW:LQ, :] = w[...]
    hold[LQ:LV, :] = q[:, 0:TILE]
    hold[LV:LP, :] = v
    hold[LP:LC, :] = p[...]
    hold[LC:LEND, :] = c[...]


def pack_kernel(*refs):
    (sm, wm, pm, qm, vm, cm, tm), rest = refs[0:7], refs[7:]
    (su, wu, pu, qu, vu, cu, tu), rest = rest[0:7], rest[7:]
    (sr, wr, pr, qr, vr), rest = rest[0:5], rest[5:]
    pack_m, pack_u = rest
    for pack, s, wt, pt, qt, vt, ct, t in (
        (pack_m, sm, wm, pm, qm, vm, cm, tm),
        (pack_u, su, wu, pu, qu, vu, cu, tu),
    ):
        pack[SRC:WAT, :] = s[...]
        pack[WAT:QAT, :] = wt[...]
        pack[QAT:VAT, :] = qt[:, 0:TILE]
        pack[VAT:MISC, :] = qt[:, TILE:]
        at = iota((8, TILE), 0)
        pack[MISC:CAT, :] = jnp.where(
            at == 0,
            jnp.broadcast_to(vt[...], (8, TILE)),
            jnp.broadcast_to(t[...].astype(F32), (8, TILE)),
        )
        pack[CAT:PAT, :] = ct[...]
        pack[PAT:END, :] = pt[...]
    pack_u[END + SRC : END + WAT, :] = sr[...]
    pack_u[END + WAT : END + QAT, :] = wr[...]
    pack_u[END + QAT : END + RMISC, :] = qr[:, 0:TILE]
    pack_u[END + RMISC : END + RPAT, :] = jnp.broadcast_to(vr[...], (8, TILE))
    pack_u[END + RPAT : END + REND, :] = pr[...]


def cross_kernel(*refs):
    _, k1, k2 = refs[HELD_REFS:]
    upper = Held(refs, END)
    root = Held(refs, END, END)
    k1[...] = cross(upper.all(PAT), upper.all(VAT))
    total = None
    for b in range(HOLD):
        p = root.one(b, RPAT)
        part = mm(p.T * root.one(b, RMISC, 1), p)
        total = part if total is None else total + part
    k2[...] = total


def leaf_up_kernel(s0, s1, s2, s3, y0, plan, rows, hold, out, z_out, zp_out, k_out):
    total = (s0[...] + s1[...]) + (s2[...] + s3[...])
    mh, mc = masks(rows, 0)
    k1 = total[2 * RHS :, :]
    hq = total[0:RHS, :] * mh
    wv = (total[RHS : 2 * RHS, :] + mm(hq, k1)) * mc
    e = -mmt(wv, hold[LC:LEND, :])
    both = jnp.concatenate([e, label_rows(plan[1:2, :])], axis=0)
    at = plan[2:3, :]
    parts = jnp.concatenate(
        [both * (at == float(k)).astype(F32) for k in range(SLOTS_LEAF)], axis=0
    )
    sent = fold(raw(stacked(parts), row_onehot(plan[0:1, :], 64).astype(BF16), 1, 1))
    sent = fill([sent], 64).T
    for place in range(HOLD):
        part = sent[HOLD * place : HOLD * (place + 1), :]
        for copy in range(HOLD):
            low = (place * HOLD + copy) * HOLD
            out[low : low + HOLD, :] = part
    p = hold[LP:LC, :]
    z = (y0[...] + mmt(hq, p)) * rows[7:8, :]
    z_out[...] = z
    zp_out[...] = mm(z, p)
    k_out[...] = k1


def write_copies(ref, value):
    rows = value.shape[0]
    for i in range(ref.shape[0] // rows):
        ref[rows * i : rows * (i + 1), :] = value


def write_shares(ref, members, value, parts):
    step = ref.shape[0] // members
    rows = step - parts.shape[0] // min(members, 16)
    each = step - rows
    common = value.shape[0] == rows
    for i in range(members):
        low = step * i
        ref[low : low + rows, :] = value if common else value[rows * i : rows * (i + 1)]
        at = each * (i % 16)
        ref[low + rows : low + step, :] = parts[at : at + each]


def sum_rows(ref, step, low, high):
    total = ref[low:high, :]
    for i in range(1, ref.shape[0] // step):
        total = total + ref[step * i + low : step * i + high, :]
    return total


def stack_rows(ref, step, low, high, count):
    return jnp.concatenate(
        [ref[step * i + low : step * i + high, :] for i in range(count)], axis=0
    )


def enter_middle_kernel(*refs):
    got, part, y_out, upd_out, scratch, sems = refs[HELD_REFS:]
    held = Fetched(refs, MISC, SRC, VAT, scratch, sems)
    inc = received(got[...].T, SLOTS_LEAF, 2 * TILE)
    held.wait()
    b = [held.one(j, SRC, RHS) + inc[RHS * j : RHS * (j + 1), 0:TILE] for j in range(HOLD)]
    write_copies(part, mm(lanes(b), held.all(QAT)))
    y_out[...] = lanes(by_tiles(b, held, WAT))
    upd_out[...] = inc[:, TILE:]


def middle_kernel(*refs):
    red, y0, rows, part, z_out, zp_out, scratch, sems = refs[HELD_REFS:]
    held = Fetched(refs, MISC, VAT, END, scratch, sems)
    mh, _ = masks(rows, 1)
    hq = sum_rows(red, RHS, 0, RHS) * mh
    held.wait()
    p, v = held.all(PAT), held.all(VAT)
    y = y0[...] + mmt(hq, p)
    write_shares(part, 8, mm(y, v), cross(p, v))
    z = y * lanes([held.one(b, MISC, 1) for b in range(HOLD)])
    z_out[...] = z
    zp_out[...] = mm(z, p)


def middle_up_kernel(*refs):
    red, upd, rows, k1, out, k_out, scratch, copied, sems = refs[HELD_REFS:]
    held = Fetched(refs, MISC, MISC, PAT, copied, sems)
    _, mc = masks(rows, 1)
    total = sum_rows(red, 3 * RHS, 0, 3 * RHS)
    k_out[...] = total[RHS:, :]
    wv = total[0:RHS, :] * mc
    held.wait()
    e = cut_lanes(mmt(wv, held.all(CAT)))
    upds = cut_tall(upd[...])
    targets = held.misc(MISC, 1).astype(jnp.int32)
    sent = messages([u - v for u, v in zip(upds, e)], targets, 14, 128, scratch)
    write_shares(out, 16, sent, k1[...])


def enter_upper_kernel(*refs):
    got, part, y_out, upd_out = refs[HELD_REFS:]
    held = Held(refs, END)
    k1 = sum_rows(got, 2 * RHS, RHS, 2 * RHS)
    inc = received(stack_rows(got, 2 * RHS, 0, RHS, 16).T, HOLD, 2 * TILE)
    b = [held.one(j, SRC, RHS) + inc[RHS * j : RHS * (j + 1), 0:TILE] for j in range(HOLD)]
    y = lanes(by_tiles(b, held, WAT))
    write_copies(part, tall([mm(lanes(b), held.all(QAT)), mm(y, held.all(VAT)), k1]))
    y_out[...] = y
    upd_out[...] = inc[:, TILE:]


def upper_up_kernel(*refs):
    red, y0, upd, rows, k2, out, z_out, zp_out, k_out, scratch = refs[HELD_REFS:]
    held = Held(refs, END)
    total = sum_rows(red, 3 * RHS, 0, 2 * RHS)
    k1 = stack_rows(red, 3 * RHS, 2 * RHS, 3 * RHS, 16)
    k_out[...] = k1
    mh, mc = masks(rows, 2)
    hq = total[0:RHS, :] * mh
    wv = (total[RHS:, :] + mm(hq, k1)) * mc
    e = cut_lanes(mmt(wv, held.all(CAT)))
    upds = cut_tall(upd[...])
    targets = held.misc(MISC, 1).astype(jnp.int32)
    sent = messages([u - v for u, v in zip(upds, e)], targets, 15, 256, scratch)
    write_shares(out, 32, sent, k2[...])
    p = held.all(PAT)
    y = y0[...] + mmt(hq, p)
    z = y * lanes([held.one(b, MISC, 1) for b in range(HOLD)])
    z_out[...] = z
    zp_out[...] = mm(z, p)


def enter_root_kernel(*refs):
    got, part, y_out = refs[HELD_REFS:]
    held = Held(refs, END, END)
    k2 = sum_rows(got, 2 * RHS, RHS, 2 * RHS)
    inc = received(stack_rows(got, 2 * RHS, 0, RHS, 32).T, HOLD, TILE)
    b = [held.one(j, SRC, RHS) + inc[RHS * j : RHS * (j + 1)] for j in range(HOLD)]
    y = lanes(by_tiles(b, held, WAT))
    z = y * lanes([held.one(j, RMISC, 1) for j in range(HOLD)])
    write_copies(part, tall([mm(lanes(b), held.all(QAT)), mm(z, held.all(RPAT)), k2]))
    y_out[...] = y


def root_kernel(*refs):
    red, y0, rows, got, answer, reply = refs[HELD_REFS:]
    held = Held(refs, END, END)
    total = sum_rows(red, 3 * RHS, 0, 2 * RHS)
    k2 = stack_rows(red, 3 * RHS, 2 * RHS, 3 * RHS, 16)
    mh = rows[6:7, :]
    hq = total[0:RHS, :] * mh
    pr = (total[RHS:, :] + mm(hq, k2)) * mh
    turned = stack_rows(got, 2 * RHS, 0, RHS, 32).T
    r = y0[...] + mmt(hq, held.all(RPAT))
    r = r * lanes([held.one(j, RMISC, 1) for j in range(HOLD)])
    x = by_tiles(cut_lanes(r), held, WAT, True)
    low = cut_lanes(mmt(pr, held.all(QAT)))
    x = [u + v for u, v in zip(x, low)]
    answer[...] = x[0]
    reply[...] = replies(turned, HOLD, tall(x))


def fetch_kernel(shift, cut, *refs):
    back, *tails, part, xu_out, scratch = refs[HELD_REFS:]
    held = Held(refs, cut)
    targets = held.misc(MISC, 1).astype(jnp.int32)
    xu = fetched(back[...], targets, shift, scratch)
    write_copies(part, tall([mm(lanes(xu), held.all(CAT))] + [ref[...] for ref in tails]))
    xu_out[...] = tall(xu)


def solve_held(total, z, k1, held, mh, mc):
    s = total[0:RHS, :] * mc
    r = z - mmt(s, held.all(VAT))
    pr = (total[RHS:, :] - mmt(s, k1)) * mh
    x = by_tiles(cut_lanes(r), held, WAT, True)
    low = cut_lanes(mmt(pr, held.all(QAT)))
    return [u + v for u, v in zip(x, low)]


def down_upper_kernel(*refs):
    red, z, rows, xu, got, k1, answer, reply = refs[HELD_REFS:]
    held = Held(refs, END)
    mh, mc = masks(rows, 2)
    total = sum_rows(red, 2 * RHS, 0, 2 * RHS)
    turned = stack_rows(got, 2 * RHS, 0, RHS, 16).T
    x = solve_held(total, z[...], k1[...], held, mh, mc)
    answer[...] = x[0]
    reply[...] = replies(turned, HOLD, jnp.concatenate([tall(x), xu[...]], axis=1))


def down_middle_kernel(*refs):
    red, z, rows, xu, got, answer, reply = refs[HELD_REFS:]
    held = Held(refs, MISC)
    mh, mc = masks(rows, 1)
    total = sum_rows(red, 4 * RHS, 0, 2 * RHS)
    k1 = stack_rows(red, 4 * RHS, 2 * RHS, 4 * RHS, 8)
    me = own_number()
    asked = [
        got[pl.ds(pl.multiple_of((HOLD * i + me) * HOLD, HOLD), HOLD), :]
        for i in range(HOLD)
    ]
    x = solve_held(total, z[...], k1, held, mh, mc)
    answer[...] = x[0]
    both = jnp.concatenate([tall(x), xu[...]], axis=1)
    reply[...] = replies(tall(asked).T, SLOTS_LEAF, both)


def fetch_leaf_kernel(back, plan, hold, zp, part):
    turned = back[...].T
    slots = tall([turned[SLOT * k : SLOT * k + RHS, :] for k in range(SLOTS_LEAF)])
    both = fold(raw(stacked(slots), row_onehot(plan[0:1, :], 64).astype(BF16), 1, 0))
    at = plan[2:3, :]
    xu = None
    for k in range(SLOTS_LEAF):
        one = both[RHS * k : RHS * (k + 1), :] * (at == float(k)).astype(F32)
        xu = one if xu is None else xu + one
    part[0:RHS, :] = mm(xu, hold[LC:LEND, :])
    part[RHS:, :] = zp[...]


def leaf_kernel(s0, s1, s2, s3, z, k1, hold, rows, answer):
    total = (s0[...] + s1[...]) + (s2[...] + s3[...])
    mh, mc = masks(rows, 0)
    s = total[0:RHS, :] * mc
    r = z[...] - mmt(s, hold[LV:LP, :])
    pr = (total[RHS:, :] - mmt(s, k1[...])) * mh
    answer[...] = mmt(r, hold[LW:LQ, :]) + mmt(pr, hold[LQ:LV, :])


def run(kernel, shapes, *args, answer=False, inputs=False, scratch=(), copied=0):
    outs = [pltpu.VMEM(s, F32) for s in shapes]
    if answer:
        outs[0] = jax.ShapeDtypeStruct(shapes[0], F32)
    options = {}
    scratch = [pltpu.VMEM(s, F32) for s in scratch]
    if copied:
        scratch += [pltpu.VMEM((HOLD, copied, TILE), F32), pltpu.SemaphoreType.DMA((12,))]
        rest = [pltpu.with_memory_space_constraint(a, pltpu.VMEM) for a in args[HELD_REFS:]]
        far = [pltpu.with_memory_space_constraint(a, pltpu.HBM) for a in args[:HELD_REFS]]
        args = far + rest
        options["in_specs"] = [pl.BlockSpec(memory_space=pltpu.HBM)] * HELD_REFS + [
            pl.BlockSpec(memory_space=pltpu.VMEM) for _ in rest
        ]
    elif not inputs:
        args = [pltpu.with_memory_space_constraint(a, pltpu.VMEM) for a in args]
    return pl.pallas_call(
        kernel,
        out_shape=outs[0] if len(outs) == 1 else outs,
        scratch_shapes=scratch,
        compiler_params=None if inputs else pltpu.CompilerParams(vmem_limit_bytes=16 << 20),
        name=getattr(kernel, "func", kernel).__name__,
        **options,
    )(*args)


def after(done, *values):
    return lax.optimization_barrier((*values, done))[:-1]


def swap(value, axis, mask):
    pairs = [(s, s ^ mask) for s in range(lax.axis_size(axis))]
    return lax.ppermute(value, axis, pairs)


def shift(value, step):
    size = lax.axis_size("grid")
    return lax.ppermute(value, "grid", [(s, (s + step) % size) for s in range(size)])


def four(value, axis, unit):
    return [value] + [swap(value, axis, unit * m) for m in (1, 2, 3)]


def add_four(values):
    return (values[0] + values[1]) + (values[2] + values[3])


def together(*values):
    return lax.optimization_barrier(values)


def between(value, members):
    size = lax.axis_size("leaf")
    groups = [
        [start + core + 2 * i for i in range(members)]
        for start in range(0, size, 2 * members)
        for core in range(2)
    ]
    return lax.all_to_all(
        value, "leaf", split_axis=0, concat_axis=0, tiled=True, axis_index_groups=groups
    )


def route_leaf(value):
    size = lax.axis_size("leaf") * lax.axis_size("grid")
    groups = [list(range(g, g + 64)) for g in range(0, size, 64)]
    return lax.all_to_all(
        value,
        ("leaf", "grid"),
        split_axis=0,
        concat_axis=0,
        tiled=True,
        axis_index_groups=groups,
    )


def shards(
    src_l, w_l, p_l, q_l, piv_l, c_l, ranks_l, t_l,
    src_m, w_m, p_m, q_m, piv_m, c_m, ranks_m, t_m,
    src_u, w_u, p_u, q_u, piv_u, c_u, ranks_u, t_u,
    src_r, w_r, p_r, q_r, piv_r, ranks_r,
):
    ranks_l, ranks_m, ranks_u, ranks_r = (r.T for r in (ranks_l, ranks_m, ranks_u, ranks_r))
    t_l, t_m, t_u = (t.reshape(1, -1) for t in (t_l, t_m, t_u))
    piv_l, piv_m, piv_u, piv_r = (v.reshape(1, -1) for v in (piv_l, piv_m, piv_u, piv_r))
    row = (RHS, TILE)
    pair = (2 * RHS, TILE)
    flat = (RHS, HOLD * TILE)
    high = (HOLD * RHS, TILE)

    first, y_l, plan, rows, hold = run(
        leaf_start_kernel,
        [(2 * RHS + TILE, TILE), row, (RHS, 2 * TILE), row, (LEND, TILE)],
        src_l, w_l, p_l, q_l, c_l, piv_l, t_l, ranks_l, ranks_m, ranks_u, ranks_r,
        inputs=True,
    )
    sums = four(first, "grid", 1)
    pack_m, pack_u = run(
        pack_kernel, [(END, TILE), (END + REND, TILE)],
        src_m, w_m, p_m, q_m, piv_m, c_m, t_m,
        src_u, w_u, p_u, q_u, piv_u, c_u, t_u,
        src_r, w_r, p_r, q_r, piv_r,
        inputs=True,
    )
    m_core, u_core = swap(pack_m, "leaf", 1), swap(pack_u, "leaf", 1)
    *sums, pack_m = together(*sums, pack_m)
    m_prev, m_next = shift(pack_m, 1), shift(pack_m, -1)
    out, z_l, zp_l, k_l = run(
        leaf_up_kernel,
        [(64 * HOLD, LANES), row, row, (TILE, TILE)],
        *sums, y_l, plan, rows, hold,
    )
    m_prev, m_next = after(out, m_prev, m_next)
    m_low, m_high, out = together(m_prev[:MISC], m_next[MISC:], out)
    m_low, m_high = shift(m_low, 1), shift(m_high, -1)
    got_m = route_leaf(out)
    m_prev_core, m_next_core = swap(m_prev, "leaf", 1), swap(m_next, "leaf", 1)
    m_low, m_high, pack_u = after(got_m, m_low, m_high, pack_u)
    u_prev, u_next = shift(pack_u, 1), shift(pack_u, -1)
    held_m = (
        pack_m, m_prev, m_next, m_low, m_high,
        m_core, m_prev_core, m_next_core, swap(m_low, "leaf", 1), swap(m_high, "leaf", 1),
    )

    part, y_m, upd_m = run(
        enter_middle_kernel, [(8 * RHS, TILE), flat, high], *held_m, got_m,
        copied=VAT - SRC,
    )
    red = between(part, 8)
    u_prev, u_next = after(red, u_prev, u_next)
    u_low, u_high = shift(u_prev[:END], 1), shift(u_next[END:], -1)
    u_prev_core, u_next_core = swap(u_prev, "leaf", 1), swap(u_next, "leaf", 1)
    part, z_m, zp_m = run(
        middle_kernel, [(8 * 3 * RHS, TILE), flat, row], *held_m, red, y_m, rows,
        copied=END - VAT,
    )
    u_low, u_high = after(part, u_low, u_high)
    held_u = (
        pack_u, u_prev, u_next, u_low, u_high,
        u_core, u_prev_core, u_next_core, swap(u_low, "leaf", 1), swap(u_high, "leaf", 1),
    )
    red = between(part, 8)
    k_u, k_r = run(cross_kernel, [(TILE, TILE)] * 2, *held_u, red)
    out, k_m = run(
        middle_up_kernel, [(16 * 2 * RHS, LANES), pair],
        *held_m, red, upd_m, rows, k_u, scratch=[(LANES, 128)], copied=PAT - MISC,
    )
    got_u = between(out, 16)

    part, y_u, upd_u = run(
        enter_upper_kernel, [(16 * 3 * RHS, TILE), flat, high], *held_u, got_u
    )
    red = between(part, 16)
    out, z_u, zp_u, k_u = run(
        upper_up_kernel, [(32 * 2 * RHS, LANES), flat, row, (TILE, TILE)],
        *held_u, red, y_u, upd_u, rows, k_r, scratch=[(LANES, 256)],
    )
    got_r = between(out, 32)

    part, y_r = run(enter_root_kernel, [(32 * 3 * RHS, TILE), flat], *held_u, got_r)
    red = between(part, 32)
    x_r, out = run(
        root_kernel, [row, (256, LANES)], *held_u, red, y_r, rows, got_r, answer=True
    )

    back = between(out, 32)
    part, xu = run(
        functools.partial(fetch_kernel, 15, END), [(16 * 2 * RHS, TILE), high],
        *held_u, back, zp_u, scratch=[(LANES, 256)],
    )
    red = between(part, 16)
    x_u, out = run(
        down_upper_kernel, [row, (128, LANES)],
        *held_u, red, z_u, rows, xu, got_u, k_u, answer=True,
    )

    back = between(out, 16)
    part, xu = run(
        functools.partial(fetch_kernel, 14, MISC), [(8 * 4 * RHS, TILE), high],
        *held_m, back, zp_m, k_m, scratch=[(LANES, 128)],
    )
    red = between(part, 8)
    x_m, out = run(
        down_middle_kernel, [row, (64, LANES)],
        *held_m, red, z_m, rows, xu, got_m, answer=True,
    )

    back = between(out, 8)
    part = run(fetch_leaf_kernel, [pair], back, plan, hold, zp_l)
    x_l = run(leaf_kernel, [row], *four(part, "grid", 1), z_l, k_l, hold, rows, answer=True)
    return (x_l, x_m, x_u, x_r)


def solution(mesh):
    both = ("leaf", "grid")
    wide = P(None, both)
    deep = P(both, None)
    line = P(both)
    level = (wide, deep, deep, deep, line, deep, P(), line)
    in_specs = level * 3 + (wide, deep, deep, deep, line, P())
    return jax.shard_map(
        shards, mesh=mesh, in_specs=in_specs, out_specs=(wide,) * 4, check_vma=False
    )
```

```python
import functools

import jax
import jax.numpy as jnp
from jax import lax
from jax.experimental import pallas as pl
from jax.experimental.pallas import tpu as pltpu
from jax.sharding import PartitionSpec as P


RHS = 8
LANES = 128
TILE = 128
HOLD = 8
SLOT = 16
SLOTS_LEAF = 4

SRC, WAT, QAT, VAT, MISC, CAT, PAT, END = 0, 8, 136, 264, 392, 400, 528, 656
RMISC, RPAT, REND = 264, 272, 400

F32 = jnp.float32
BF16 = jnp.bfloat16


def iota(shape, dim):
    return lax.broadcasted_iota(jnp.int32, shape, dim)


def raw(a, b, ca, cb):
    return lax.dot_general(a, b, (((ca,), (cb,)), ((), ())), preferred_element_type=F32)


def halves(a):
    high = a.astype(BF16)
    low = (a - high.astype(F32)).astype(BF16)
    return high, low


def stacked(a):
    high = a.astype(BF16).astype(F32)
    return jnp.concatenate([high, a - high], axis=0).astype(BF16)


def fold(total):
    rows = total.shape[0] // 2
    return total[0:rows] + total[rows:]


def dot(a, b, ca, cb):
    high, low = halves(b)
    both = stacked(a)
    return fold(raw(both, high, ca, cb) + raw(both, low, ca, cb))


def mm(a, b):
    return dot(a, b, 1, 0)


def mmt(a, b):
    return dot(a, b, 1, 1)


def cross(a, b):
    a_high, a_low = halves(a)
    b_high, b_low = halves(b)
    return (raw(a_low, b_high, 0, 0) + raw(a_high, b_low, 0, 0)) + raw(a_high, b_high, 0, 0)


def mask_rows(ranks_ref, groups, fronts_dim):
    front = lax.axis_index("leaf") // groups
    both = ranks_ref[...].astype(F32)
    own = iota(both.shape, fronts_dim) == front
    pair = jnp.sum(jnp.where(own, both, 0.0), axis=fronts_dim, keepdims=True)
    lane = iota((1, TILE), 1).astype(F32)
    if fronts_dim == 0:
        return [(lane < pair[:, i : i + 1]).astype(F32) for i in range(2)]
    return [(lane < pair[i : i + 1, :]).astype(F32) for i in range(2)]


def masks(rows_ref, level):
    return rows_ref[2 * level : 2 * level + 1, :], rows_ref[2 * level + 1 : 2 * level + 2, :]


def split_target(targets, shift):
    piece = lax.shift_right_logical(targets, shift)
    within = jnp.bitwise_and(targets, (1 << shift) - 1)
    dest = lax.shift_right_logical(within, 7)
    label = piece * TILE + jnp.bitwise_and(within, TILE - 1)
    return dest, label.astype(F32)


def row_onehot(at, count):
    n = at.shape[1]
    if at.dtype == jnp.int32:
        rows = iota((count, n), 0)
    else:
        rows = iota((count, n), 0).astype(F32)
    return (rows == jnp.broadcast_to(at, (count, n))).astype(F32)


def leaf_slots(onehot):
    n = onehot.shape[1]
    upper = (iota((n, n), 0) <= iota((n, n), 1)).astype(BF16)
    order = raw(onehot.astype(BF16), upper, 1, 0)
    return jnp.sum(order * onehot, axis=0, keepdims=True) - 1.0


def label_rows(label):
    n = label.shape[1]
    return jnp.where(iota((SLOT - RHS, n), 0) == 0, jnp.broadcast_to(label, (SLOT - RHS, n)), 0.0)


def fill(rows, n):
    used = sum(r.shape[0] for r in rows)
    if used < LANES:
        rows = rows + [jnp.zeros((LANES - used, n), F32)]
    return jnp.concatenate(rows, axis=0)


def block_mask(n):
    lane = jnp.bitwise_and(iota((RHS, n), 1), HOLD - 1)
    return jnp.concatenate([(lane == at).astype(F32) for at in numbers()], axis=0)


def received(turned, slots, cols):
    n = turned.shape[1]
    mask = block_mask(n)
    total = None
    for k in range(slots):
        values = turned[SLOT * k : SLOT * k + RHS, :]
        label = turned[SLOT * k + RHS : SLOT * k + RHS + 1, :]
        spread = jnp.concatenate([values] * HOLD, axis=0) * mask
        part = raw(stacked(spread), row_onehot(label, cols).astype(BF16), 1, 1)
        total = part if total is None else total + part
    return fold(total)


def replies(turned, slots, rows):
    n = turned.shape[1]
    mask = block_mask(n)
    both = stacked(rows)
    out = []
    for k in range(slots):
        label = turned[SLOT * k + RHS : SLOT * k + RHS + 1, :]
        found = fold(raw(both, row_onehot(label, rows.shape[1]).astype(BF16), 1, 0)) * mask
        one = found[0:RHS]
        for j in range(1, HOLD):
            one = one + found[RHS * j : RHS * (j + 1)]
        out += [one, jnp.zeros((SLOT - RHS, n), F32)]
    return fill(out, n).T


def slot_rows(at):
    return pl.ds(pl.multiple_of(SLOT * at, SLOT), SLOT)


def messages(blocks, targets, shift, count, scratch):
    for r, at in enumerate(numbers()):
        dest, label = split_target(targets[r : r + 1], shift)
        one = jnp.concatenate([blocks[r], label_rows(label)], axis=0)
        found = fold(raw(stacked(one), row_onehot(dest, count).astype(BF16), 1, 1))
        scratch[slot_rows(at), :] = found
    return scratch[...].T


def fetched(back, targets, shift, scratch):
    scratch[...] = back.T
    count = scratch.shape[1]
    out = []
    for r, at in enumerate(numbers()):
        dest, _ = split_target(targets[r : r + 1], shift)
        values = scratch[slot_rows(at), :][0:RHS]
        out.append(fold(raw(stacked(values), row_onehot(dest, count).astype(BF16), 1, 0)))
    return out


def lanes(blocks):
    return jnp.concatenate(blocks, axis=1)


def tall(blocks):
    return jnp.concatenate(blocks, axis=0)


def cut_lanes(value):
    return [value[:, TILE * b : TILE * (b + 1)] for b in range(HOLD)]


def cut_tall(value):
    return [value[RHS * b : RHS * (b + 1)] for b in range(HOLD)]


def own_number():
    core = jnp.bitwise_and(lax.axis_index("leaf"), 1)
    return core * 4 + lax.axis_index("grid")


def numbers():
    core = jnp.bitwise_and(lax.axis_index("leaf"), 1)
    at = lax.axis_index("grid")
    out = []
    for c in (core, 1 - core):
        for step in (0, 3, 1, 2):
            out.append(c * 4 + jnp.bitwise_and(at + step, 3))
    return out


class Held:
    def __init__(self, refs, cut, base=0):
        own, prev, after, low, high = refs[0:5]
        self.own = (own, prev, after)
        self.opposite = (low, high)
        self.core = refs[5:8]
        self.core_opposite = refs[8:10]
        self.cut = cut
        self.base = base

    def one(self, b, at, rows=TILE):
        at = at + self.base
        singles, split = (
            (self.own, self.opposite) if b < 4 else (self.core, self.core_opposite)
        )
        if b % 4 < 3:
            ref = singles[b % 4]
        elif at < self.cut:
            ref = split[0]
        else:
            ref = split[1]
            at = at - self.cut
        return ref[at : at + rows, :]

    def all(self, at):
        return jnp.concatenate([self.one(b, at) for b in range(HOLD)], axis=0)

    def misc(self, at, row):
        return jnp.concatenate([self.one(b, at + row, 1) for b in range(HOLD)], axis=0)


class Fetched(Held):
    def __init__(self, refs, cut, low, high, scratch, sems):
        self.low = low
        self.scratch = scratch
        self.copies = []
        own, core = refs[0:5], refs[5:10]
        for half, bufs in enumerate((own, core)):
            for b in range(3):
                self.start(bufs[b], low, low, high, 4 * half + b, sems)
            if low < cut:
                self.start(bufs[3], low, low, min(high, cut), 4 * half + 3, sems)
            if high > cut:
                at = max(low, cut)
                self.start(bufs[4], at - cut, at, high, 4 * half + 3, sems)

    def start(self, buf, source, low, high, b, sems):
        copy = pltpu.make_async_copy(
            buf.at[pl.ds(source, high - low)],
            self.scratch.at[b, pl.ds(low - self.low, high - low)],
            sems.at[len(self.copies)],
        )
        copy.start()
        self.copies.append(copy)

    def wait(self):
        for copy in self.copies:
            copy.wait()

    def one(self, b, at, rows=TILE):
        return self.scratch[b, at - self.low : at - self.low + rows, :]


def by_tiles(blocks, held, at, turned=False):
    return [
        dot(blocks[b], held.one(b, at), 1, 1 if turned else 0) for b in range(HOLD)
    ]


HELD_REFS = 10


LW, LQ, LV, LP, LC, LEND = 0, 128, 256, 384, 512, 768


def leaf_start_kernel(
    src, w, p, q, c, piv, tl, ranks_l, ranks_m, ranks_u, ranks_r,
    first, y0, plan, rows, hold,
):
    b = src[...]
    y = mm(b, w[...])
    v = q[:, TILE:]
    first[0:RHS, :] = mm(b, q[:, 0:TILE])
    first[RHS : 2 * RHS, :] = mm(y, v)
    first[2 * RHS :, :] = cross(p[...], v)
    y0[...] = y
    dest, label = split_target(tl[...], 13)
    plan[0:1, :] = dest.astype(F32)
    plan[1:2, :] = label
    plan[2:3, :] = leaf_slots(row_onehot(dest, 64))
    plan[3:8, :] = jnp.zeros((5, 2 * TILE), F32)
    found = []
    for ranks, groups, dim in (
        (ranks_l, 1, 1), (ranks_m, 16, 1), (ranks_u, 32, 0), (ranks_r, 64, 0),
    ):
        found += mask_rows(ranks, groups, dim)
    rows[...] = jnp.concatenate(found[0:7] + [piv[...]], axis=0)
    hold[LW:LQ, :] = w[...]
    hold[LQ:LV, :] = q[:, 0:TILE]
    hold[LV:LP, :] = v
    hold[LP:LC, :] = p[...]
    hold[LC:LEND, :] = c[...]


def pack_kernel(*refs):
    (sm, wm, pm, qm, vm, cm, tm), rest = refs[0:7], refs[7:]
    (su, wu, pu, qu, vu, cu, tu), rest = rest[0:7], rest[7:]
    (sr, wr, pr, qr, vr), rest = rest[0:5], rest[5:]
    pack_m, pack_u = rest
    for pack, s, wt, pt, qt, vt, ct, t in (
        (pack_m, sm, wm, pm, qm, vm, cm, tm),
        (pack_u, su, wu, pu, qu, vu, cu, tu),
    ):
        pack[SRC:WAT, :] = s[...]
        pack[WAT:QAT, :] = wt[...]
        pack[QAT:VAT, :] = qt[:, 0:TILE]
        pack[VAT:MISC, :] = qt[:, TILE:]
        at = iota((8, TILE), 0)
        pack[MISC:CAT, :] = jnp.where(
            at == 0,
            jnp.broadcast_to(vt[...], (8, TILE)),
            jnp.broadcast_to(t[...].astype(F32), (8, TILE)),
        )
        pack[CAT:PAT, :] = ct[...]
        pack[PAT:END, :] = pt[...]
    pack_u[END + SRC : END + WAT, :] = sr[...]
    pack_u[END + WAT : END + QAT, :] = wr[...]
    pack_u[END + QAT : END + RMISC, :] = qr[:, 0:TILE]
    pack_u[END + RMISC : END + RPAT, :] = jnp.broadcast_to(vr[...], (8, TILE))
    pack_u[END + RPAT : END + REND, :] = pr[...]


def cross_kernel(*refs):
    _, k1, k2, low, high, low_core, high_core = refs[HELD_REFS:]
    for source, kept in zip(refs[3:5] + refs[8:10], (low, high, low_core, high_core)):
        kept[...] = source[...]
    upper = Held(refs, END)
    root = Held(refs, END, END)
    k1[...] = cross(upper.all(PAT), upper.all(VAT))
    total = None
    for b in range(HOLD):
        p = root.one(b, RPAT)
        part = mm(p.T * root.one(b, RMISC, 1), p)
        total = part if total is None else total + part
    k2[...] = total


def leaf_up_kernel(s0, s1, s2, s3, y0, plan, rows, hold, out, z_out, zp_out, k_out):
    total = (s0[...] + s1[...]) + (s2[...] + s3[...])
    mh, mc = masks(rows, 0)
    k1 = total[2 * RHS :, :]
    hq = total[0:RHS, :] * mh
    wv = (total[RHS : 2 * RHS, :] + mm(hq, k1)) * mc
    e = -mmt(wv, hold[LC:LEND, :])
    both = jnp.concatenate([e, label_rows(plan[1:2, :])], axis=0)
    at = plan[2:3, :]
    parts = jnp.concatenate(
        [both * (at == float(k)).astype(F32) for k in range(SLOTS_LEAF)], axis=0
    )
    sent = fold(raw(stacked(parts), row_onehot(plan[0:1, :], 64).astype(BF16), 1, 1))
    sent = fill([sent], 64).T
    for place in range(HOLD):
        part = sent[HOLD * place : HOLD * (place + 1), :]
        for copy in range(HOLD):
            low = (place * HOLD + copy) * HOLD
            out[low : low + HOLD, :] = part
    p = hold[LP:LC, :]
    z = (y0[...] + mmt(hq, p)) * rows[7:8, :]
    z_out[...] = z
    zp_out[...] = mm(z, p)
    k_out[...] = k1


def write_copies(ref, value):
    rows = value.shape[0]
    for i in range(ref.shape[0] // rows):
        ref[rows * i : rows * (i + 1), :] = value


def write_shares(ref, members, value, parts):
    step = ref.shape[0] // members
    rows = step - parts.shape[0] // min(members, 16)
    each = step - rows
    common = value.shape[0] == rows
    for i in range(members):
        low = step * i
        ref[low : low + rows, :] = value if common else value[rows * i : rows * (i + 1)]
        at = each * (i % 16)
        ref[low + rows : low + step, :] = parts[at : at + each]


def sum_rows(ref, step, low, high):
    total = ref[low:high, :]
    for i in range(1, ref.shape[0] // step):
        total = total + ref[step * i + low : step * i + high, :]
    return total


def stack_rows(ref, step, low, high, count):
    return jnp.concatenate(
        [ref[step * i + low : step * i + high, :] for i in range(count)], axis=0
    )


def enter_middle_kernel(*refs):
    got, part, y_out, upd_out, scratch, sems = refs[HELD_REFS:]
    held = Fetched(refs, MISC, SRC, VAT, scratch, sems)
    inc = received(got[...].T, SLOTS_LEAF, 2 * TILE)
    held.wait()
    b = [held.one(j, SRC, RHS) + inc[RHS * j : RHS * (j + 1), 0:TILE] for j in range(HOLD)]
    write_copies(part, mm(lanes(b), held.all(QAT)))
    y_out[...] = lanes(by_tiles(b, held, WAT))
    upd_out[...] = inc[:, TILE:]


def middle_kernel(*refs):
    red, y0, rows, part, z_out, zp_out, scratch, sems = refs[HELD_REFS:]
    held = Fetched(refs, MISC, VAT, END, scratch, sems)
    mh, _ = masks(rows, 1)
    hq = sum_rows(red, RHS, 0, RHS) * mh
    held.wait()
    p, v = held.all(PAT), held.all(VAT)
    y = y0[...] + mmt(hq, p)
    write_shares(part, 8, mm(y, v), cross(p, v))
    z = y * lanes([held.one(b, MISC, 1) for b in range(HOLD)])
    z_out[...] = z
    zp_out[...] = mm(z, p)


def middle_up_kernel(*refs):
    red, upd, rows, k1, out, k_out, scratch, copied, sems = refs[HELD_REFS:]
    held = Fetched(refs, MISC, MISC, PAT, copied, sems)
    _, mc = masks(rows, 1)
    total = sum_rows(red, 3 * RHS, 0, 3 * RHS)
    k_out[...] = total[RHS:, :]
    wv = total[0:RHS, :] * mc
    held.wait()
    e = cut_lanes(mmt(wv, held.all(CAT)))
    upds = cut_tall(upd[...])
    targets = held.misc(MISC, 1).astype(jnp.int32)
    sent = messages([u - v for u, v in zip(upds, e)], targets, 14, 128, scratch)
    write_shares(out, 16, sent, k1[...])


def enter_upper_kernel(*refs):
    got, part, y_out, upd_out = refs[HELD_REFS:]
    held = Held(refs, END)
    k1 = sum_rows(got, 2 * RHS, RHS, 2 * RHS)
    inc = received(stack_rows(got, 2 * RHS, 0, RHS, 16).T, HOLD, 2 * TILE)
    b = [held.one(j, SRC, RHS) + inc[RHS * j : RHS * (j + 1), 0:TILE] for j in range(HOLD)]
    y = lanes(by_tiles(b, held, WAT))
    write_copies(part, tall([mm(lanes(b), held.all(QAT)), mm(y, held.all(VAT)), k1]))
    y_out[...] = y
    upd_out[...] = inc[:, TILE:]


def upper_up_kernel(*refs):
    red, y0, upd, rows, k2, out, z_out, zp_out, k_out, scratch = refs[HELD_REFS:]
    held = Held(refs, END)
    total = sum_rows(red, 3 * RHS, 0, 2 * RHS)
    k1 = stack_rows(red, 3 * RHS, 2 * RHS, 3 * RHS, 16)
    k_out[...] = k1
    mh, mc = masks(rows, 2)
    hq = total[0:RHS, :] * mh
    wv = (total[RHS:, :] + mm(hq, k1)) * mc
    e = cut_lanes(mmt(wv, held.all(CAT)))
    upds = cut_tall(upd[...])
    targets = held.misc(MISC, 1).astype(jnp.int32)
    sent = messages([u - v for u, v in zip(upds, e)], targets, 15, 256, scratch)
    write_shares(out, 32, sent, k2[...])
    p = held.all(PAT)
    y = y0[...] + mmt(hq, p)
    z = y * lanes([held.one(b, MISC, 1) for b in range(HOLD)])
    z_out[...] = z
    zp_out[...] = mm(z, p)


def enter_root_kernel(*refs):
    got, part, y_out = refs[HELD_REFS:]
    held = Held(refs, END, END)
    k2 = sum_rows(got, 2 * RHS, RHS, 2 * RHS)
    inc = received(stack_rows(got, 2 * RHS, 0, RHS, 32).T, HOLD, TILE)
    b = [held.one(j, SRC, RHS) + inc[RHS * j : RHS * (j + 1)] for j in range(HOLD)]
    y = lanes(by_tiles(b, held, WAT))
    z = y * lanes([held.one(j, RMISC, 1) for j in range(HOLD)])
    write_copies(part, tall([mm(lanes(b), held.all(QAT)), mm(z, held.all(RPAT)), k2]))
    y_out[...] = y


def root_kernel(*refs):
    red, y0, rows, got, answer, reply = refs[HELD_REFS:]
    held = Held(refs, END, END)
    total = sum_rows(red, 3 * RHS, 0, 2 * RHS)
    k2 = stack_rows(red, 3 * RHS, 2 * RHS, 3 * RHS, 16)
    mh = rows[6:7, :]
    hq = total[0:RHS, :] * mh
    pr = (total[RHS:, :] + mm(hq, k2)) * mh
    turned = stack_rows(got, 2 * RHS, 0, RHS, 32).T
    r = y0[...] + mmt(hq, held.all(RPAT))
    r = r * lanes([held.one(j, RMISC, 1) for j in range(HOLD)])
    x = by_tiles(cut_lanes(r), held, WAT, True)
    low = cut_lanes(mmt(pr, held.all(QAT)))
    x = [u + v for u, v in zip(x, low)]
    answer[...] = x[0]
    reply[...] = replies(turned, HOLD, tall(x))


def fetch_kernel(shift, cut, *refs):
    back, *tails, part, xu_out, scratch = refs[HELD_REFS:]
    held = Held(refs, cut)
    targets = held.misc(MISC, 1).astype(jnp.int32)
    xu = fetched(back[...], targets, shift, scratch)
    write_copies(part, tall([mm(lanes(xu), held.all(CAT))] + [ref[...] for ref in tails]))
    xu_out[...] = tall(xu)


def solve_held(total, z, k1, held, mh, mc):
    s = total[0:RHS, :] * mc
    r = z - mmt(s, held.all(VAT))
    pr = (total[RHS:, :] - mmt(s, k1)) * mh
    x = by_tiles(cut_lanes(r), held, WAT, True)
    low = cut_lanes(mmt(pr, held.all(QAT)))
    return [u + v for u, v in zip(x, low)]


def down_upper_kernel(*refs):
    red, z, rows, xu, got, k1, answer, reply = refs[HELD_REFS:]
    held = Held(refs, END)
    mh, mc = masks(rows, 2)
    total = sum_rows(red, 2 * RHS, 0, 2 * RHS)
    turned = stack_rows(got, 2 * RHS, 0, RHS, 16).T
    x = solve_held(total, z[...], k1[...], held, mh, mc)
    answer[...] = x[0]
    reply[...] = replies(turned, HOLD, jnp.concatenate([tall(x), xu[...]], axis=1))


def down_middle_kernel(*refs):
    red, z, rows, xu, got, answer, reply = refs[HELD_REFS:]
    held = Held(refs, MISC)
    mh, mc = masks(rows, 1)
    total = sum_rows(red, 4 * RHS, 0, 2 * RHS)
    k1 = stack_rows(red, 4 * RHS, 2 * RHS, 4 * RHS, 8)
    me = own_number()
    asked = [
        got[pl.ds(pl.multiple_of((HOLD * i + me) * HOLD, HOLD), HOLD), :]
        for i in range(HOLD)
    ]
    x = solve_held(total, z[...], k1, held, mh, mc)
    answer[...] = x[0]
    both = jnp.concatenate([tall(x), xu[...]], axis=1)
    reply[...] = replies(tall(asked).T, SLOTS_LEAF, both)


def fetch_leaf_kernel(back, plan, hold, zp, part):
    turned = back[...].T
    slots = tall([turned[SLOT * k : SLOT * k + RHS, :] for k in range(SLOTS_LEAF)])
    both = fold(raw(stacked(slots), row_onehot(plan[0:1, :], 64).astype(BF16), 1, 0))
    at = plan[2:3, :]
    xu = None
    for k in range(SLOTS_LEAF):
        one = both[RHS * k : RHS * (k + 1), :] * (at == float(k)).astype(F32)
        xu = one if xu is None else xu + one
    part[0:RHS, :] = mm(xu, hold[LC:LEND, :])
    part[RHS:, :] = zp[...]


def leaf_kernel(s0, s1, s2, s3, z, k1, hold, rows, answer):
    total = (s0[...] + s1[...]) + (s2[...] + s3[...])
    mh, mc = masks(rows, 0)
    s = total[0:RHS, :] * mc
    r = z[...] - mmt(s, hold[LV:LP, :])
    pr = (total[RHS:, :] - mmt(s, k1[...])) * mh
    answer[...] = mmt(r, hold[LW:LQ, :]) + mmt(pr, hold[LQ:LV, :])


def run(kernel, shapes, *args, answer=False, inputs=False, scratch=(), copied=0):
    outs = [pltpu.VMEM(s, F32) for s in shapes]
    if answer:
        outs[0] = jax.ShapeDtypeStruct(shapes[0], F32)
    options = {}
    scratch = [pltpu.VMEM(s, F32) for s in scratch]
    if copied:
        scratch += [pltpu.VMEM((HOLD, copied, TILE), F32), pltpu.SemaphoreType.DMA((12,))]
        rest = [pltpu.with_memory_space_constraint(a, pltpu.VMEM) for a in args[HELD_REFS:]]
        far = [pltpu.with_memory_space_constraint(a, pltpu.HBM) for a in args[:HELD_REFS]]
        args = far + rest
        options["in_specs"] = [pl.BlockSpec(memory_space=pltpu.HBM)] * HELD_REFS + [
            pl.BlockSpec(memory_space=pltpu.VMEM) for _ in rest
        ]
    elif not inputs:
        args = [pltpu.with_memory_space_constraint(a, pltpu.VMEM) for a in args]
    return pl.pallas_call(
        kernel,
        out_shape=outs[0] if len(outs) == 1 else outs,
        scratch_shapes=scratch,
        compiler_params=None if inputs else pltpu.CompilerParams(vmem_limit_bytes=16 << 20),
        **options,
    )(*args)


def after(done, *values):
    return lax.optimization_barrier((*values, done))[:-1]


def swap(value, axis, mask):
    pairs = [(s, s ^ mask) for s in range(lax.axis_size(axis))]
    return lax.ppermute(value, axis, pairs)


def shift(value, step):
    size = lax.axis_size("grid")
    return lax.ppermute(value, "grid", [(s, (s + step) % size) for s in range(size)])


def four(value, axis, unit):
    return [value] + [swap(value, axis, unit * m) for m in (1, 2, 3)]


def together(*values):
    return lax.optimization_barrier(values)


def between(value, members):
    size = lax.axis_size("leaf")
    groups = [
        [start + core + 2 * i for i in range(members)]
        for start in range(0, size, 2 * members)
        for core in range(2)
    ]
    return lax.all_to_all(
        value, "leaf", split_axis=0, concat_axis=0, tiled=True, axis_index_groups=groups
    )


def route_leaf(value):
    size = lax.axis_size("leaf") * lax.axis_size("grid")
    groups = [list(range(g, g + 64)) for g in range(0, size, 64)]
    return lax.all_to_all(
        value,
        ("leaf", "grid"),
        split_axis=0,
        concat_axis=0,
        tiled=True,
        axis_index_groups=groups,
    )


def shards(
    src_l, w_l, p_l, q_l, piv_l, c_l, ranks_l, t_l,
    src_m, w_m, p_m, q_m, piv_m, c_m, ranks_m, t_m,
    src_u, w_u, p_u, q_u, piv_u, c_u, ranks_u, t_u,
    src_r, w_r, p_r, q_r, piv_r, ranks_r,
):
    ranks_l, ranks_m = ranks_l.T, ranks_m.T
    t_l, t_m, t_u = (t.reshape(1, -1) for t in (t_l, t_m, t_u))
    piv_l, piv_m, piv_u, piv_r = (v.reshape(1, -1) for v in (piv_l, piv_m, piv_u, piv_r))
    row = (RHS, TILE)
    pair = (2 * RHS, TILE)
    flat = (RHS, HOLD * TILE)
    high = (HOLD * RHS, TILE)

    first, y_l, plan, rows, hold = run(
        leaf_start_kernel,
        [(2 * RHS + TILE, TILE), row, (RHS, 2 * TILE), row, (LEND, TILE)],
        src_l, w_l, p_l, q_l, c_l, piv_l, t_l, ranks_l, ranks_m, ranks_u, ranks_r,
        inputs=True,
    )
    sums = four(first, "grid", 1)
    pack_m, pack_u = run(
        pack_kernel, [(END, TILE), (END + REND, TILE)],
        src_m, w_m, p_m, q_m, piv_m, c_m, t_m,
        src_u, w_u, p_u, q_u, piv_u, c_u, t_u,
        src_r, w_r, p_r, q_r, piv_r,
        inputs=True,
    )
    m_core, u_core = swap(pack_m, "leaf", 1), swap(pack_u, "leaf", 1)
    *sums, pack_m = together(*sums, pack_m)
    m_prev = shift(pack_m, 1)
    m_next = shift(pack_m, -1)
    out, z_l, zp_l, k_l = run(
        leaf_up_kernel,
        [(64 * HOLD, LANES), row, row, (TILE, TILE)],
        *sums, y_l, plan, rows, hold,
    )
    got_m = route_leaf(out)
    m_prev, m_next, pack_u = after(got_m, m_prev, m_next, pack_u)
    m_low, m_high = shift(m_prev[:MISC], 1), shift(m_next[MISC:], -1)
    m_prev_core, m_next_core = swap(m_prev, "leaf", 1), swap(m_next, "leaf", 1)
    m_low, m_high, pack_u = together(m_low, m_high, pack_u)
    u_prev, u_next = shift(pack_u, 1), shift(pack_u, -1)
    held_m = (
        pack_m, m_prev, m_next, m_low, m_high,
        m_core, m_prev_core, m_next_core, swap(m_low, "leaf", 1), swap(m_high, "leaf", 1),
    )

    part, y_m, upd_m = run(
        enter_middle_kernel, [(8 * RHS, TILE), flat, high], *held_m, got_m,
        copied=VAT - SRC,
    )
    red = between(part, 8)
    u_prev, u_next = after(red, u_prev, u_next)
    u_low, u_high = shift(u_prev[:END], 1), shift(u_next[END:], -1)
    u_prev_core, u_next_core = swap(u_prev, "leaf", 1), swap(u_next, "leaf", 1)
    part, z_m, zp_m = run(
        middle_kernel, [(8 * 3 * RHS, TILE), flat, row], *held_m, red, y_m, rows,
        copied=END - VAT,
    )
    u_low, u_high = after(part, u_low, u_high)
    held_u = (
        pack_u, u_prev, u_next, u_low, u_high,
        u_core, u_prev_core, u_next_core, swap(u_low, "leaf", 1), swap(u_high, "leaf", 1),
    )
    red = between(part, 8)
    k_u, k_r, *opposite = run(
        cross_kernel, [(TILE, TILE)] * 2 + [(END, TILE), (REND, TILE)] * 2, *held_u, red
    )
    held_u = (*held_u[:3], *opposite[:2], *held_u[5:8], *opposite[2:])
    out, k_m = run(
        middle_up_kernel, [(16 * 2 * RHS, LANES), pair],
        *held_m, red, upd_m, rows, k_u, scratch=[(LANES, 128)], copied=PAT - MISC,
    )
    got_u = between(out, 16)

    part, y_u, upd_u = run(
        enter_upper_kernel, [(16 * 3 * RHS, TILE), flat, high], *held_u, got_u
    )
    red = between(part, 16)
    out, z_u, zp_u, k_u = run(
        upper_up_kernel, [(32 * 2 * RHS, LANES), flat, row, (TILE, TILE)],
        *held_u, red, y_u, upd_u, rows, k_r, scratch=[(LANES, 256)],
    )
    got_r = between(out, 32)

    part, y_r = run(enter_root_kernel, [(32 * 3 * RHS, TILE), flat], *held_u, got_r)
    red = between(part, 32)
    x_r, out = run(
        root_kernel, [row, (256, LANES)], *held_u, red, y_r, rows, got_r, answer=True
    )

    back = between(out, 32)
    part, xu = run(
        functools.partial(fetch_kernel, 15, END), [(16 * 2 * RHS, TILE), high],
        *held_u, back, zp_u, scratch=[(LANES, 256)],
    )
    red = between(part, 16)
    x_u, out = run(
        down_upper_kernel, [row, (128, LANES)],
        *held_u, red, z_u, rows, xu, got_u, k_u, answer=True,
    )

    back = between(out, 16)
    part, xu = run(
        functools.partial(fetch_kernel, 14, MISC), [(8 * 4 * RHS, TILE), high],
        *held_m, back, zp_m, k_m, scratch=[(LANES, 128)],
    )
    red = between(part, 8)
    x_m, out = run(
        down_middle_kernel, [row, (64, LANES)],
        *held_m, red, z_m, rows, xu, got_m, answer=True,
    )

    back = between(out, 8)
    part = run(fetch_leaf_kernel, [pair], back, plan, hold, zp_l)
    x_l = run(leaf_kernel, [row], *four(part, "grid", 1), z_l, k_l, hold, rows, answer=True)
    return (x_l, x_m, x_u, x_r)


def solution(mesh):
    both = ("leaf", "grid")
    wide = P(None, both)
    deep = P(both, None)
    line = P(both)
    level = (wide, deep, deep, deep, line, deep, P(), line)
    in_specs = level * 3 + (wide, deep, deep, deep, line, P())
    return jax.shard_map(
        shards, mesh=mesh, in_specs=in_specs, out_specs=(wide,) * 4, check_vma=False
    )
```

```python
import functools

import jax
import jax.numpy as jnp
from jax import lax
from jax.experimental import pallas as pl
from jax.experimental.pallas import tpu as pltpu
from jax.sharding import PartitionSpec as P


RHS = 8
LANES = 128
TILE = 128
HOLD = 8
SLOT = 16
SLOTS_LEAF = 4

SRC, WAT, QAT, VAT, MISC, CAT, PAT, END = 0, 8, 136, 264, 392, 400, 528, 656
RMISC, RPAT, REND = 264, 272, 400

F32 = jnp.float32
BF16 = jnp.bfloat16


def iota(shape, dim):
    return lax.broadcasted_iota(jnp.int32, shape, dim)


def raw(a, b, ca, cb):
    return lax.dot_general(a, b, (((ca,), (cb,)), ((), ())), preferred_element_type=F32)


def halves(a):
    high = a.astype(BF16)
    low = (a - high.astype(F32)).astype(BF16)
    return high, low


def stacked(a):
    high = a.astype(BF16).astype(F32)
    return jnp.concatenate([high, a - high], axis=0).astype(BF16)


def fold(total):
    rows = total.shape[0] // 2
    return total[0:rows] + total[rows:]


def dot(a, b, ca, cb):
    high, low = halves(b)
    both = stacked(a)
    return fold(raw(both, high, ca, cb) + raw(both, low, ca, cb))


def mm(a, b):
    return dot(a, b, 1, 0)


def mmt(a, b):
    return dot(a, b, 1, 1)


def cross(a, b):
    a_high, a_low = halves(a)
    b_high, b_low = halves(b)
    return (raw(a_low, b_high, 0, 0) + raw(a_high, b_low, 0, 0)) + raw(a_high, b_high, 0, 0)


def mask_rows(ranks_ref, groups, fronts_dim):
    front = lax.axis_index("leaf") // groups
    both = ranks_ref[...].astype(F32)
    own = iota(both.shape, fronts_dim) == front
    pair = jnp.sum(jnp.where(own, both, 0.0), axis=fronts_dim, keepdims=True)
    lane = iota((1, TILE), 1).astype(F32)
    if fronts_dim == 0:
        return [(lane < pair[:, i : i + 1]).astype(F32) for i in range(2)]
    return [(lane < pair[i : i + 1, :]).astype(F32) for i in range(2)]


def masks(rows_ref, level):
    return rows_ref[2 * level : 2 * level + 1, :], rows_ref[2 * level + 1 : 2 * level + 2, :]


def split_target(targets, shift):
    piece = lax.shift_right_logical(targets, shift)
    within = jnp.bitwise_and(targets, (1 << shift) - 1)
    dest = lax.shift_right_logical(within, 7)
    label = piece * TILE + jnp.bitwise_and(within, TILE - 1)
    return dest, label.astype(F32)


def row_onehot(at, count):
    n = at.shape[1]
    if at.dtype == jnp.int32:
        rows = iota((count, n), 0)
    else:
        rows = iota((count, n), 0).astype(F32)
    return (rows == jnp.broadcast_to(at, (count, n))).astype(F32)


def leaf_slots(onehot):
    n = onehot.shape[1]
    upper = (iota((n, n), 0) <= iota((n, n), 1)).astype(BF16)
    order = raw(onehot.astype(BF16), upper, 1, 0)
    return jnp.sum(order * onehot, axis=0, keepdims=True) - 1.0


def label_rows(label):
    n = label.shape[1]
    return jnp.where(iota((SLOT - RHS, n), 0) == 0, jnp.broadcast_to(label, (SLOT - RHS, n)), 0.0)


def fill(rows, n):
    used = sum(r.shape[0] for r in rows)
    if used < LANES:
        rows = rows + [jnp.zeros((LANES - used, n), F32)]
    return jnp.concatenate(rows, axis=0)


def block_mask(n, half=None):
    if half is None:
        lane = jnp.bitwise_and(iota((RHS, n), 1), HOLD - 1)
    else:
        lane = jnp.bitwise_and(iota((RHS, n), 1), 3) + 4 * half
    return jnp.concatenate([(lane == at).astype(F32) for at in numbers()], axis=0)


def slot_masks(n, halves_of):
    if halves_of:
        return [block_mask(n, k // SLOTS_LEAF) for k in range(2 * SLOTS_LEAF)]
    return [block_mask(n)] * HOLD


def received(turned, halves_of, cols):
    total = None
    for k, mask in enumerate(slot_masks(turned.shape[1], halves_of)):
        values = turned[SLOT * k : SLOT * k + RHS, :]
        label = turned[SLOT * k + RHS : SLOT * k + RHS + 1, :]
        spread = jnp.concatenate([values] * HOLD, axis=0) * mask
        part = raw(stacked(spread), row_onehot(label, cols).astype(BF16), 1, 1)
        total = part if total is None else total + part
    return fold(total)


def replies(turned, halves_of, rows):
    n = turned.shape[1]
    both = stacked(rows)
    out = []
    for k, mask in enumerate(slot_masks(n, halves_of)):
        label = turned[SLOT * k + RHS : SLOT * k + RHS + 1, :]
        found = fold(raw(both, row_onehot(label, rows.shape[1]).astype(BF16), 1, 0)) * mask
        one = found[0:RHS]
        for j in range(1, HOLD):
            one = one + found[RHS * j : RHS * (j + 1)]
        out += [one, jnp.zeros((SLOT - RHS, n), F32)]
    return fill(out, n).T


def slot_rows(at):
    return pl.ds(pl.multiple_of(SLOT * at, SLOT), SLOT)


def messages(blocks, targets, shift, count, scratch):
    for r, at in enumerate(numbers()):
        dest, label = split_target(targets[r : r + 1], shift)
        one = jnp.concatenate([blocks[r], label_rows(label)], axis=0)
        found = fold(raw(stacked(one), row_onehot(dest, count).astype(BF16), 1, 1))
        scratch[slot_rows(at), :] = found
    return scratch[...].T


def fetched(back, targets, shift, scratch):
    scratch[...] = back.T
    count = scratch.shape[1]
    out = []
    for r, at in enumerate(numbers()):
        dest, _ = split_target(targets[r : r + 1], shift)
        values = scratch[slot_rows(at), :][0:RHS]
        out.append(fold(raw(stacked(values), row_onehot(dest, count).astype(BF16), 1, 0)))
    return out


def lanes(blocks):
    return jnp.concatenate(blocks, axis=1)


def tall(blocks):
    return jnp.concatenate(blocks, axis=0)


def cut_lanes(value):
    return [value[:, TILE * b : TILE * (b + 1)] for b in range(HOLD)]


def cut_tall(value):
    return [value[RHS * b : RHS * (b + 1)] for b in range(HOLD)]


def own_number():
    core = jnp.bitwise_and(lax.axis_index("leaf"), 1)
    return core * 4 + lax.axis_index("grid")


def numbers():
    core = jnp.bitwise_and(lax.axis_index("leaf"), 1)
    at = lax.axis_index("grid")
    out = []
    for c in (core, 1 - core):
        for step in (0, 3, 1, 2):
            out.append(c * 4 + jnp.bitwise_and(at + step, 3))
    return out


class Held:
    def __init__(self, refs, cut, base=0):
        own, prev, after, low, high = refs[0:5]
        self.own = (own, prev, after)
        self.opposite = (low, high)
        self.core = refs[5:8]
        self.core_opposite = refs[8:10]
        self.cut = cut
        self.base = base

    def one(self, b, at, rows=TILE):
        at = at + self.base
        singles, split = (
            (self.own, self.opposite) if b < 4 else (self.core, self.core_opposite)
        )
        if b % 4 < 3:
            ref = singles[b % 4]
        elif at < self.cut:
            ref = split[0]
        else:
            ref = split[1]
            at = at - self.cut
        return ref[at : at + rows, :]

    def all(self, at):
        return jnp.concatenate([self.one(b, at) for b in range(HOLD)], axis=0)

    def misc(self, at, row):
        return jnp.concatenate([self.one(b, at + row, 1) for b in range(HOLD)], axis=0)


class Fetched(Held):
    def __init__(self, refs, cut, low, high, scratch, sems):
        self.low = low
        self.scratch = scratch
        self.copies = []
        own, core = refs[0:5], refs[5:10]
        for half, bufs in enumerate((own, core)):
            for b in range(3):
                self.start(bufs[b], low, low, high, 4 * half + b, sems)
            if low < cut:
                self.start(bufs[3], low, low, min(high, cut), 4 * half + 3, sems)
            if high > cut:
                at = max(low, cut)
                self.start(bufs[4], at - cut, at, high, 4 * half + 3, sems)

    def start(self, buf, source, low, high, b, sems):
        copy = pltpu.make_async_copy(
            buf.at[pl.ds(source, high - low)],
            self.scratch.at[b, pl.ds(low - self.low, high - low)],
            sems.at[len(self.copies)],
        )
        copy.start()
        self.copies.append(copy)

    def wait(self):
        for copy in self.copies:
            copy.wait()

    def one(self, b, at, rows=TILE):
        return self.scratch[b, at - self.low : at - self.low + rows, :]


def by_tiles(blocks, held, at, turned=False):
    return [
        dot(blocks[b], held.one(b, at), 1, 1 if turned else 0) for b in range(HOLD)
    ]


HELD_REFS = 10


LW, LQ, LV, LP, LC, LEND = 0, 128, 256, 384, 512, 768


def leaf_start_kernel(
    src, w, p, q, c, piv, tl, ranks_l, ranks_m, ranks_u, ranks_r,
    first, y0, plan, rows, hold,
):
    b = src[...]
    y = mm(b, w[...])
    v = q[:, TILE:]
    first[0:RHS, :] = mm(b, q[:, 0:TILE])
    first[RHS : 2 * RHS, :] = mm(y, v)
    first[2 * RHS :, :] = cross(p[...], v)
    y0[...] = y
    dest, label = split_target(tl[...], 13)
    plan[0:1, :] = dest.astype(F32)
    plan[1:2, :] = label
    plan[2:3, :] = leaf_slots(row_onehot(dest, 64))
    plan[3:8, :] = jnp.zeros((5, 2 * TILE), F32)
    found = []
    for ranks, groups, dim in (
        (ranks_l, 1, 1), (ranks_m, 16, 1), (ranks_u, 32, 0), (ranks_r, 64, 0),
    ):
        found += mask_rows(ranks, groups, dim)
    rows[...] = jnp.concatenate(found[0:7] + [piv[...]], axis=0)
    hold[LW:LQ, :] = w[...]
    hold[LQ:LV, :] = q[:, 0:TILE]
    hold[LV:LP, :] = v
    hold[LP:LC, :] = p[...]
    hold[LC:LEND, :] = c[...]


def pack_kernel(*refs):
    (sm, wm, pm, qm, vm, cm, tm), rest = refs[0:7], refs[7:]
    (su, wu, pu, qu, vu, cu, tu), rest = rest[0:7], rest[7:]
    (sr, wr, pr, qr, vr), rest = rest[0:5], rest[5:]
    pack_m, pack_u = rest
    for pack, s, wt, pt, qt, vt, ct, t in (
        (pack_m, sm, wm, pm, qm, vm, cm, tm),
        (pack_u, su, wu, pu, qu, vu, cu, tu),
    ):
        pack[SRC:WAT, :] = s[...]
        pack[WAT:QAT, :] = wt[...]
        pack[QAT:VAT, :] = qt[:, 0:TILE]
        pack[VAT:MISC, :] = qt[:, TILE:]
        at = iota((8, TILE), 0)
        pack[MISC:CAT, :] = jnp.where(
            at == 0,
            jnp.broadcast_to(vt[...], (8, TILE)),
            jnp.broadcast_to(t[...].astype(F32), (8, TILE)),
        )
        pack[CAT:PAT, :] = ct[...]
        pack[PAT:END, :] = pt[...]
    pack_u[END + SRC : END + WAT, :] = sr[...]
    pack_u[END + WAT : END + QAT, :] = wr[...]
    pack_u[END + QAT : END + RMISC, :] = qr[:, 0:TILE]
    pack_u[END + RMISC : END + RPAT, :] = jnp.broadcast_to(vr[...], (8, TILE))
    pack_u[END + RPAT : END + REND, :] = pr[...]


def cross_kernel(*refs):
    _, k1, k2, low, high, low_core, high_core = refs[HELD_REFS:]
    for source, kept in zip(refs[3:5] + refs[8:10], (low, high, low_core, high_core)):
        kept[...] = source[...]
    upper = Held(refs, END)
    root = Held(refs, END, END)
    k1[...] = cross(upper.all(PAT), upper.all(VAT))
    total = None
    for b in range(HOLD):
        p = root.one(b, RPAT)
        part = mm(p.T * root.one(b, RMISC, 1), p)
        total = part if total is None else total + part
    k2[...] = total


def leaf_picks(plan):
    dest = plan[0:1, :].astype(jnp.int32)
    place = lax.shift_right_logical(dest, 3) * 4 + jnp.bitwise_and(dest, 3)
    half = jnp.bitwise_and(lax.shift_right_logical(dest, 2), 1)
    hit = row_onehot(place, 4 * HOLD)
    return [hit * (half == h).astype(F32) for h in range(2)]


def leaf_up_kernel(s0, s1, s2, s3, y0, plan, rows, hold, out, z_out, zp_out, k_out):
    total = (s0[...] + s1[...]) + (s2[...] + s3[...])
    mh, mc = masks(rows, 0)
    k1 = total[2 * RHS :, :]
    hq = total[0:RHS, :] * mh
    wv = (total[RHS : 2 * RHS, :] + mm(hq, k1)) * mc
    e = -mmt(wv, hold[LC:LEND, :])
    both = jnp.concatenate([e, label_rows(plan[1:2, :])], axis=0)
    at = plan[2:3, :]
    parts = jnp.concatenate(
        [both * (at == float(k)).astype(F32) for k in range(SLOTS_LEAF)], axis=0
    )
    both = stacked(parts)
    sent = tall([fold(raw(both, pick.astype(BF16), 1, 1)) for pick in leaf_picks(plan)]).T
    for place in range(0, HOLD, 2):
        pairs = [sent[4 * at : 4 * at + 4, :] for at in (place, place + 1)]
        for at, part in zip((place, place + 1), pairs):
            twice = jnp.concatenate([part, part], axis=0)
            for copy in range(0, HOLD, 2):
                low = (at * HOLD + copy) * 4
                out[low : low + HOLD, :] = twice
    p = hold[LP:LC, :]
    z = (y0[...] + mmt(hq, p)) * rows[7:8, :]
    z_out[...] = z
    zp_out[...] = mm(z, p)
    k_out[...] = k1


def write_copies(ref, value):
    rows = value.shape[0]
    for i in range(ref.shape[0] // rows):
        ref[rows * i : rows * (i + 1), :] = value


def write_shares(ref, members, value, parts):
    step = ref.shape[0] // members
    rows = step - parts.shape[0] // min(members, 16)
    each = step - rows
    common = value.shape[0] == rows
    for i in range(members):
        low = step * i
        ref[low : low + rows, :] = value if common else value[rows * i : rows * (i + 1)]
        at = each * (i % 16)
        ref[low + rows : low + step, :] = parts[at : at + each]


def sum_rows(ref, step, low, high):
    total = ref[low:high, :]
    for i in range(1, ref.shape[0] // step):
        total = total + ref[step * i + low : step * i + high, :]
    return total


def stack_rows(ref, step, low, high, count):
    return jnp.concatenate(
        [ref[step * i + low : step * i + high, :] for i in range(count)], axis=0
    )


def enter_middle_kernel(*refs):
    got, part, y_out, upd_out, scratch, sems = refs[HELD_REFS:]
    held = Fetched(refs, MISC, SRC, VAT, scratch, sems)
    inc = received(got[...].T, True, 2 * TILE)
    held.wait()
    b = [held.one(j, SRC, RHS) + inc[RHS * j : RHS * (j + 1), 0:TILE] for j in range(HOLD)]
    write_copies(part, mm(lanes(b), held.all(QAT)))
    y_out[...] = lanes(by_tiles(b, held, WAT))
    upd_out[...] = inc[:, TILE:]


def middle_kernel(*refs):
    red, y0, rows, part, z_out, zp_out, scratch, sems = refs[HELD_REFS:]
    held = Fetched(refs, MISC, VAT, END, scratch, sems)
    mh, _ = masks(rows, 1)
    hq = sum_rows(red, RHS, 0, RHS) * mh
    held.wait()
    p, v = held.all(PAT), held.all(VAT)
    y = y0[...] + mmt(hq, p)
    write_shares(part, 8, mm(y, v), cross(p, v))
    z = y * lanes([held.one(b, MISC, 1) for b in range(HOLD)])
    z_out[...] = z
    zp_out[...] = mm(z, p)


def middle_up_kernel(*refs):
    red, upd, rows, k1, out, k_out, scratch, copied, sems = refs[HELD_REFS:]
    held = Fetched(refs, MISC, MISC, PAT, copied, sems)
    _, mc = masks(rows, 1)
    total = sum_rows(red, 3 * RHS, 0, 3 * RHS)
    k_out[...] = total[RHS:, :]
    wv = total[0:RHS, :] * mc
    held.wait()
    e = cut_lanes(mmt(wv, held.all(CAT)))
    upds = cut_tall(upd[...])
    targets = held.misc(MISC, 1).astype(jnp.int32)
    sent = messages([u - v for u, v in zip(upds, e)], targets, 14, 128, scratch)
    write_shares(out, 16, sent, k1[...])


def enter_upper_kernel(*refs):
    got, part, y_out, upd_out = refs[HELD_REFS:]
    held = Held(refs, END)
    k1 = sum_rows(got, 2 * RHS, RHS, 2 * RHS)
    inc = received(stack_rows(got, 2 * RHS, 0, RHS, 16).T, False, 2 * TILE)
    b = [held.one(j, SRC, RHS) + inc[RHS * j : RHS * (j + 1), 0:TILE] for j in range(HOLD)]
    y = lanes(by_tiles(b, held, WAT))
    write_copies(part, tall([mm(lanes(b), held.all(QAT)), mm(y, held.all(VAT)), k1]))
    y_out[...] = y
    upd_out[...] = inc[:, TILE:]


def upper_up_kernel(*refs):
    red, y0, upd, rows, k2, out, z_out, zp_out, k_out, scratch = refs[HELD_REFS:]
    held = Held(refs, END)
    total = sum_rows(red, 3 * RHS, 0, 2 * RHS)
    k1 = stack_rows(red, 3 * RHS, 2 * RHS, 3 * RHS, 16)
    k_out[...] = k1
    mh, mc = masks(rows, 2)
    hq = total[0:RHS, :] * mh
    wv = (total[RHS:, :] + mm(hq, k1)) * mc
    e = cut_lanes(mmt(wv, held.all(CAT)))
    upds = cut_tall(upd[...])
    targets = held.misc(MISC, 1).astype(jnp.int32)
    sent = messages([u - v for u, v in zip(upds, e)], targets, 15, 256, scratch)
    write_shares(out, 32, sent, k2[...])
    p = held.all(PAT)
    y = y0[...] + mmt(hq, p)
    z = y * lanes([held.one(b, MISC, 1) for b in range(HOLD)])
    z_out[...] = z
    zp_out[...] = mm(z, p)


def enter_root_kernel(*refs):
    got, part, y_out = refs[HELD_REFS:]
    held = Held(refs, END, END)
    k2 = sum_rows(got, 2 * RHS, RHS, 2 * RHS)
    inc = received(stack_rows(got, 2 * RHS, 0, RHS, 32).T, False, TILE)
    b = [held.one(j, SRC, RHS) + inc[RHS * j : RHS * (j + 1)] for j in range(HOLD)]
    y = lanes(by_tiles(b, held, WAT))
    z = y * lanes([held.one(j, RMISC, 1) for j in range(HOLD)])
    write_copies(part, tall([mm(lanes(b), held.all(QAT)), mm(z, held.all(RPAT)), k2]))
    y_out[...] = y


def root_kernel(*refs):
    red, y0, rows, got, answer, reply = refs[HELD_REFS:]
    held = Held(refs, END, END)
    total = sum_rows(red, 3 * RHS, 0, 2 * RHS)
    k2 = stack_rows(red, 3 * RHS, 2 * RHS, 3 * RHS, 16)
    mh = rows[6:7, :]
    hq = total[0:RHS, :] * mh
    pr = (total[RHS:, :] + mm(hq, k2)) * mh
    turned = stack_rows(got, 2 * RHS, 0, RHS, 32).T
    r = y0[...] + mmt(hq, held.all(RPAT))
    r = r * lanes([held.one(j, RMISC, 1) for j in range(HOLD)])
    x = by_tiles(cut_lanes(r), held, WAT, True)
    low = cut_lanes(mmt(pr, held.all(QAT)))
    x = [u + v for u, v in zip(x, low)]
    answer[...] = x[0]
    reply[...] = replies(turned, False, tall(x))


def fetch_kernel(shift, cut, *refs):
    back, *tails, part, xu_out, scratch = refs[HELD_REFS:]
    held = Held(refs, cut)
    targets = held.misc(MISC, 1).astype(jnp.int32)
    xu = fetched(back[...], targets, shift, scratch)
    write_copies(part, tall([mm(lanes(xu), held.all(CAT))] + [ref[...] for ref in tails]))
    xu_out[...] = tall(xu)


def solve_held(total, z, k1, held, mh, mc):
    s = total[0:RHS, :] * mc
    r = z - mmt(s, held.all(VAT))
    pr = (total[RHS:, :] - mmt(s, k1)) * mh
    x = by_tiles(cut_lanes(r), held, WAT, True)
    low = cut_lanes(mmt(pr, held.all(QAT)))
    return [u + v for u, v in zip(x, low)]


def down_upper_kernel(*refs):
    red, z, rows, xu, got, k1, answer, reply = refs[HELD_REFS:]
    held = Held(refs, END)
    mh, mc = masks(rows, 2)
    total = sum_rows(red, 2 * RHS, 0, 2 * RHS)
    turned = stack_rows(got, 2 * RHS, 0, RHS, 16).T
    x = solve_held(total, z[...], k1[...], held, mh, mc)
    answer[...] = x[0]
    reply[...] = replies(turned, False, jnp.concatenate([tall(x), xu[...]], axis=1))


def down_middle_kernel(*refs):
    red, z, rows, xu, got, answer, reply = refs[HELD_REFS:]
    held = Held(refs, MISC)
    mh, mc = masks(rows, 1)
    total = sum_rows(red, 4 * RHS, 0, 2 * RHS)
    k1 = stack_rows(red, 4 * RHS, 2 * RHS, 4 * RHS, 8)
    me = own_number()
    pair = lax.shift_right_logical(me, 1)
    odd = jnp.bitwise_and(me, 1) == 1
    asked = []
    for i in range(HOLD):
        two = got[pl.ds(pl.multiple_of((4 * i + pair) * HOLD, HOLD), HOLD), :]
        asked.append(jnp.where(odd, two[4:], two[0:4]))
    x = solve_held(total, z[...], k1, held, mh, mc)
    answer[...] = x[0]
    both = jnp.concatenate([tall(x), xu[...]], axis=1)
    reply[...] = replies(tall(asked).T, True, both)


def fetch_leaf_kernel(back, plan, hold, zp, part):
    turned = back[...].T
    both = None
    for h, pick in enumerate(leaf_picks(plan)):
        first = h * SLOTS_LEAF
        slots = tall(
            [turned[SLOT * k : SLOT * k + RHS, :] for k in range(first, first + SLOTS_LEAF)]
        )
        one = fold(raw(stacked(slots), pick.astype(BF16), 1, 0))
        both = one if both is None else both + one
    at = plan[2:3, :]
    xu = None
    for k in range(SLOTS_LEAF):
        one = both[RHS * k : RHS * (k + 1), :] * (at == float(k)).astype(F32)
        xu = one if xu is None else xu + one
    part[0:RHS, :] = mm(xu, hold[LC:LEND, :])
    part[RHS:, :] = zp[...]


def leaf_kernel(s0, s1, s2, s3, z, k1, hold, rows, answer):
    total = (s0[...] + s1[...]) + (s2[...] + s3[...])
    mh, mc = masks(rows, 0)
    s = total[0:RHS, :] * mc
    r = z[...] - mmt(s, hold[LV:LP, :])
    pr = (total[RHS:, :] - mmt(s, k1[...])) * mh
    answer[...] = mmt(r, hold[LW:LQ, :]) + mmt(pr, hold[LQ:LV, :])


def run(kernel, shapes, *args, answer=False, inputs=False, scratch=(), copied=0):
    outs = [pltpu.VMEM(s, F32) for s in shapes]
    if answer:
        outs[0] = jax.ShapeDtypeStruct(shapes[0], F32)
    options = {}
    scratch = [pltpu.VMEM(s, F32) for s in scratch]
    if copied:
        scratch += [pltpu.VMEM((HOLD, copied, TILE), F32), pltpu.SemaphoreType.DMA((12,))]
        rest = [pltpu.with_memory_space_constraint(a, pltpu.VMEM) for a in args[HELD_REFS:]]
        far = [pltpu.with_memory_space_constraint(a, pltpu.HBM) for a in args[:HELD_REFS]]
        args = far + rest
        options["in_specs"] = [pl.BlockSpec(memory_space=pltpu.HBM)] * HELD_REFS + [
            pl.BlockSpec(memory_space=pltpu.VMEM) for _ in rest
        ]
    elif not inputs:
        args = [pltpu.with_memory_space_constraint(a, pltpu.VMEM) for a in args]
    return pl.pallas_call(
        kernel,
        out_shape=outs[0] if len(outs) == 1 else outs,
        scratch_shapes=scratch,
        compiler_params=None if inputs else pltpu.CompilerParams(vmem_limit_bytes=16 << 20),
        **options,
    )(*args)


def after(done, *values):
    return lax.optimization_barrier((*values, done))[:-1]


def swap(value, axis, mask):
    pairs = [(s, s ^ mask) for s in range(lax.axis_size(axis))]
    return lax.ppermute(value, axis, pairs)


def shift(value, step):
    size = lax.axis_size("grid")
    return lax.ppermute(value, "grid", [(s, (s + step) % size) for s in range(size)])


def four(value, axis, unit):
    return [value] + [swap(value, axis, unit * m) for m in (1, 2, 3)]


def together(*values):
    return lax.optimization_barrier(values)


def between(value, members):
    size = lax.axis_size("leaf")
    groups = [
        [start + core + 2 * i for i in range(members)]
        for start in range(0, size, 2 * members)
        for core in range(2)
    ]
    return lax.all_to_all(
        value, "leaf", split_axis=0, concat_axis=0, tiled=True, axis_index_groups=groups
    )


def route_leaf(value):
    size = lax.axis_size("leaf") * lax.axis_size("grid")
    groups = [list(range(g, g + 64)) for g in range(0, size, 64)]
    return lax.all_to_all(
        value,
        ("leaf", "grid"),
        split_axis=0,
        concat_axis=0,
        tiled=True,
        axis_index_groups=groups,
    )


def shards(
    src_l, w_l, p_l, q_l, piv_l, c_l, ranks_l, t_l,
    src_m, w_m, p_m, q_m, piv_m, c_m, ranks_m, t_m,
    src_u, w_u, p_u, q_u, piv_u, c_u, ranks_u, t_u,
    src_r, w_r, p_r, q_r, piv_r, ranks_r,
):
    ranks_l, ranks_m = ranks_l.T, ranks_m.T
    t_l, t_m, t_u = (t.reshape(1, -1) for t in (t_l, t_m, t_u))
    piv_l, piv_m, piv_u, piv_r = (v.reshape(1, -1) for v in (piv_l, piv_m, piv_u, piv_r))
    row = (RHS, TILE)
    pair = (2 * RHS, TILE)
    flat = (RHS, HOLD * TILE)
    high = (HOLD * RHS, TILE)

    first, y_l, plan, rows, hold = run(
        leaf_start_kernel,
        [(2 * RHS + TILE, TILE), row, (RHS, 2 * TILE), row, (LEND, TILE)],
        src_l, w_l, p_l, q_l, c_l, piv_l, t_l, ranks_l, ranks_m, ranks_u, ranks_r,
        inputs=True,
    )
    sums = four(first, "grid", 1)
    pack_m, pack_u = run(
        pack_kernel, [(END, TILE), (END + REND, TILE)],
        src_m, w_m, p_m, q_m, piv_m, c_m, t_m,
        src_u, w_u, p_u, q_u, piv_u, c_u, t_u,
        src_r, w_r, p_r, q_r, piv_r,
        inputs=True,
    )
    m_core, u_core = swap(pack_m, "leaf", 1), swap(pack_u, "leaf", 1)
    *sums, pack_m = together(*sums, pack_m)
    m_prev = shift(pack_m, 1)
    m_next = shift(pack_m, -1)
    out, z_l, zp_l, k_l = run(
        leaf_up_kernel,
        [(64 * 4, LANES), row, row, (TILE, TILE)],
        *sums, y_l, plan, rows, hold,
    )
    got_m = route_leaf(out)
    m_prev, m_next = after(got_m, m_prev, m_next)
    m_low, m_high = shift(m_prev[:MISC], 1), shift(m_next[MISC:], -1)
    m_prev_core, m_next_core = swap(m_prev, "leaf", 1), swap(m_next, "leaf", 1)
    held_m = (
        pack_m, m_prev, m_next, m_low, m_high,
        m_core, m_prev_core, m_next_core, swap(m_low, "leaf", 1), swap(m_high, "leaf", 1),
    )

    part, y_m, upd_m = run(
        enter_middle_kernel, [(8 * RHS, TILE), flat, high], *held_m, got_m,
        copied=VAT - SRC,
    )
    (pack_u,) = after(part, pack_u)
    u_prev = shift(pack_u, 1)
    u_next = shift(pack_u, -1)
    red = between(part, 8)
    u_prev, u_next = after(red, u_prev, u_next)
    u_low, u_high = shift(u_prev[:END], 1), shift(u_next[END:], -1)
    u_prev_core, u_next_core = swap(u_prev, "leaf", 1), swap(u_next, "leaf", 1)
    part, z_m, zp_m = run(
        middle_kernel, [(8 * 3 * RHS, TILE), flat, row], *held_m, red, y_m, rows,
        copied=END - VAT,
    )
    u_low, u_high = after(part, u_low, u_high)
    held_u = (
        pack_u, u_prev, u_next, u_low, u_high,
        u_core, u_prev_core, u_next_core, swap(u_low, "leaf", 1), swap(u_high, "leaf", 1),
    )
    red = between(part, 8)
    k_u, k_r, *opposite = run(
        cross_kernel, [(TILE, TILE)] * 2 + [(END, TILE), (REND, TILE)] * 2, *held_u, red
    )
    held_u = (*held_u[:3], *opposite[:2], *held_u[5:8], *opposite[2:])
    out, k_m = run(
        middle_up_kernel, [(16 * 2 * RHS, LANES), pair],
        *held_m, red, upd_m, rows, k_u, scratch=[(LANES, 128)], copied=PAT - MISC,
    )
    got_u = between(out, 16)

    part, y_u, upd_u = run(
        enter_upper_kernel, [(16 * 3 * RHS, TILE), flat, high], *held_u, got_u
    )
    red = between(part, 16)
    out, z_u, zp_u, k_u = run(
        upper_up_kernel, [(32 * 2 * RHS, LANES), flat, row, (TILE, TILE)],
        *held_u, red, y_u, upd_u, rows, k_r, scratch=[(LANES, 256)],
    )
    got_r = between(out, 32)

    part, y_r = run(enter_root_kernel, [(32 * 3 * RHS, TILE), flat], *held_u, got_r)
    red = between(part, 32)
    x_r, out = run(
        root_kernel, [row, (256, LANES)], *held_u, red, y_r, rows, got_r, answer=True
    )

    back = between(out, 32)
    part, xu = run(
        functools.partial(fetch_kernel, 15, END), [(16 * 2 * RHS, TILE), high],
        *held_u, back, zp_u, scratch=[(LANES, 256)],
    )
    red = between(part, 16)
    x_u, out = run(
        down_upper_kernel, [row, (128, LANES)],
        *held_u, red, z_u, rows, xu, got_u, k_u, answer=True,
    )

    back = between(out, 16)
    part, xu = run(
        functools.partial(fetch_kernel, 14, MISC), [(8 * 4 * RHS, TILE), high],
        *held_m, back, zp_m, k_m, scratch=[(LANES, 128)],
    )
    red = between(part, 8)
    x_m, out = run(
        down_middle_kernel, [row, (32, LANES)],
        *held_m, red, z_m, rows, xu, got_m, answer=True,
    )

    back = between(out, 8)
    part = run(fetch_leaf_kernel, [pair], back, plan, hold, zp_l)
    x_l = run(leaf_kernel, [row], *four(part, "grid", 1), z_l, k_l, hold, rows, answer=True)
    return (x_l, x_m, x_u, x_r)


def solution(mesh):
    both = ("leaf", "grid")
    wide = P(None, both)
    deep = P(both, None)
    line = P(both)
    level = (wide, deep, deep, deep, line, deep, P(), line)
    in_specs = level * 3 + (wide, deep, deep, deep, line, P())
    return jax.shard_map(
        shards, mesh=mesh, in_specs=in_specs, out_specs=(wide,) * 4, check_vma=False
    )
```

```python
import functools

import jax
import jax.numpy as jnp
from jax import lax
from jax.experimental import pallas as pl
from jax.experimental.pallas import tpu as pltpu
from jax.sharding import PartitionSpec as P


RHS = 8
LANES = 128
TILE = 128
HOLD = 8
SLOT = 16
SLOTS_LEAF = 4

SRC, WAT, QAT, VAT, MISC, CAT, PAT, END = 0, 8, 136, 264, 392, 400, 528, 656
RMISC, RPAT, REND = 264, 272, 400

F32 = jnp.float32
BF16 = jnp.bfloat16


def iota(shape, dim):
    return lax.broadcasted_iota(jnp.int32, shape, dim)


def raw(a, b, ca, cb):
    return lax.dot_general(a, b, (((ca,), (cb,)), ((), ())), preferred_element_type=F32)


def halves(a):
    high = a.astype(BF16)
    low = (a - high.astype(F32)).astype(BF16)
    return high, low


def stacked(a):
    high = a.astype(BF16).astype(F32)
    return jnp.concatenate([high, a - high], axis=0).astype(BF16)


def fold(total):
    rows = total.shape[0] // 2
    return total[0:rows] + total[rows:]


def dot(a, b, ca, cb):
    high, low = halves(b)
    both = stacked(a)
    return fold(raw(both, high, ca, cb) + raw(both, low, ca, cb))


def mm(a, b):
    return dot(a, b, 1, 0)


def mmt(a, b):
    return dot(a, b, 1, 1)


def cross(a, b):
    a_high, a_low = halves(a)
    b_high, b_low = halves(b)
    return (raw(a_low, b_high, 0, 0) + raw(a_high, b_low, 0, 0)) + raw(a_high, b_high, 0, 0)


def mask_rows(ranks_ref, groups, fronts_dim):
    front = lax.axis_index("leaf") // groups
    both = ranks_ref[...].astype(F32)
    own = iota(both.shape, fronts_dim) == front
    pair = jnp.sum(jnp.where(own, both, 0.0), axis=fronts_dim, keepdims=True)
    lane = iota((1, TILE), 1).astype(F32)
    if fronts_dim == 0:
        return [(lane < pair[:, i : i + 1]).astype(F32) for i in range(2)]
    return [(lane < pair[i : i + 1, :]).astype(F32) for i in range(2)]


def masks(rows_ref, level):
    return rows_ref[2 * level : 2 * level + 1, :], rows_ref[2 * level + 1 : 2 * level + 2, :]


def split_target(targets, shift):
    piece = lax.shift_right_logical(targets, shift)
    within = jnp.bitwise_and(targets, (1 << shift) - 1)
    dest = lax.shift_right_logical(within, 7)
    label = piece * TILE + jnp.bitwise_and(within, TILE - 1)
    return dest, label.astype(F32)


def row_onehot(at, count):
    n = at.shape[1]
    if at.dtype == jnp.int32:
        rows = iota((count, n), 0)
    else:
        rows = iota((count, n), 0).astype(F32)
    return (rows == jnp.broadcast_to(at, (count, n))).astype(F32)


def leaf_slots(onehot):
    n = onehot.shape[1]
    upper = (iota((n, n), 0) <= iota((n, n), 1)).astype(BF16)
    order = raw(onehot.astype(BF16), upper, 1, 0)
    return jnp.sum(order * onehot, axis=0, keepdims=True) - 1.0


def label_rows(label):
    n = label.shape[1]
    return jnp.where(iota((SLOT - RHS, n), 0) == 0, jnp.broadcast_to(label, (SLOT - RHS, n)), 0.0)


def fill(rows, n):
    used = sum(r.shape[0] for r in rows)
    if used < LANES:
        rows = rows + [jnp.zeros((LANES - used, n), F32)]
    return jnp.concatenate(rows, axis=0)


def block_mask(n, half=None):
    if half is None:
        lane = jnp.bitwise_and(iota((RHS, n), 1), HOLD - 1)
    else:
        lane = jnp.bitwise_and(iota((RHS, n), 1), 3) + 4 * half
    return jnp.concatenate([(lane == at).astype(F32) for at in numbers()], axis=0)


def slot_masks(n, halves_of):
    if halves_of:
        return [block_mask(n, k // SLOTS_LEAF) for k in range(2 * SLOTS_LEAF)]
    return [block_mask(n)] * HOLD


def received(turned, halves_of, cols):
    total = None
    for k, mask in enumerate(slot_masks(turned.shape[1], halves_of)):
        values = turned[SLOT * k : SLOT * k + RHS, :]
        label = turned[SLOT * k + RHS : SLOT * k + RHS + 1, :]
        spread = jnp.concatenate([values] * HOLD, axis=0) * mask
        part = raw(stacked(spread), row_onehot(label, cols).astype(BF16), 1, 1)
        total = part if total is None else total + part
    return fold(total)


def replies(turned, halves_of, rows):
    n = turned.shape[1]
    both = stacked(rows)
    out = []
    for k, mask in enumerate(slot_masks(n, halves_of)):
        label = turned[SLOT * k + RHS : SLOT * k + RHS + 1, :]
        found = fold(raw(both, row_onehot(label, rows.shape[1]).astype(BF16), 1, 0)) * mask
        one = found[0:RHS]
        for j in range(1, HOLD):
            one = one + found[RHS * j : RHS * (j + 1)]
        out += [one, jnp.zeros((SLOT - RHS, n), F32)]
    return fill(out, n).T


def slot_rows(at):
    return pl.ds(pl.multiple_of(SLOT * at, SLOT), SLOT)


def messages(blocks, targets, shift, count, scratch):
    for r, at in enumerate(numbers()):
        dest, label = split_target(targets[r : r + 1], shift)
        one = jnp.concatenate([blocks[r], label_rows(label)], axis=0)
        found = fold(raw(stacked(one), row_onehot(dest, count).astype(BF16), 1, 1))
        scratch[slot_rows(at), :] = found
    return scratch[...].T


def fetched(back, targets, shift, scratch):
    scratch[...] = back.T
    count = scratch.shape[1]
    out = []
    for r, at in enumerate(numbers()):
        dest, _ = split_target(targets[r : r + 1], shift)
        values = scratch[slot_rows(at), :][0:RHS]
        out.append(fold(raw(stacked(values), row_onehot(dest, count).astype(BF16), 1, 0)))
    return out


def lanes(blocks):
    return jnp.concatenate(blocks, axis=1)


def tall(blocks):
    return jnp.concatenate(blocks, axis=0)


def cut_lanes(value):
    return [value[:, TILE * b : TILE * (b + 1)] for b in range(HOLD)]


def cut_tall(value):
    return [value[RHS * b : RHS * (b + 1)] for b in range(HOLD)]


def own_number():
    core = jnp.bitwise_and(lax.axis_index("leaf"), 1)
    return core * 4 + lax.axis_index("grid")


def numbers():
    core = jnp.bitwise_and(lax.axis_index("leaf"), 1)
    at = lax.axis_index("grid")
    out = []
    for c in (core, 1 - core):
        for step in (0, 3, 1, 2):
            out.append(c * 4 + jnp.bitwise_and(at + step, 3))
    return out


class Held:
    def __init__(self, refs, cut, base=0):
        own, prev, after, low, high = refs[0:5]
        self.own = (own, prev, after)
        self.opposite = (low, high)
        self.core = refs[5:8]
        self.core_opposite = refs[8:10]
        self.cut = cut
        self.base = base

    def one(self, b, at, rows=TILE):
        at = at + self.base
        singles, split = (
            (self.own, self.opposite) if b < 4 else (self.core, self.core_opposite)
        )
        if b % 4 < 3:
            ref = singles[b % 4]
        elif at < self.cut:
            ref = split[0]
        else:
            ref = split[1]
            at = at - self.cut
        return ref[at : at + rows, :]

    def all(self, at):
        return jnp.concatenate([self.one(b, at) for b in range(HOLD)], axis=0)

    def misc(self, at, row):
        return jnp.concatenate([self.one(b, at + row, 1) for b in range(HOLD)], axis=0)


class Fetched(Held):
    def __init__(self, refs, cut, low, high, scratch, sems):
        self.low = low
        self.scratch = scratch
        self.copies = []
        own, core = refs[0:5], refs[5:10]
        for half, bufs in enumerate((own, core)):
            for b in range(3):
                self.start(bufs[b], low, low, high, 4 * half + b, sems)
            if low < cut:
                self.start(bufs[3], low, low, min(high, cut), 4 * half + 3, sems)
            if high > cut:
                at = max(low, cut)
                self.start(bufs[4], at - cut, at, high, 4 * half + 3, sems)

    def start(self, buf, source, low, high, b, sems):
        copy = pltpu.make_async_copy(
            buf.at[pl.ds(source, high - low)],
            self.scratch.at[b, pl.ds(low - self.low, high - low)],
            sems.at[len(self.copies)],
        )
        copy.start()
        self.copies.append(copy)

    def wait(self):
        for copy in self.copies:
            copy.wait()

    def one(self, b, at, rows=TILE):
        return self.scratch[b, at - self.low : at - self.low + rows, :]


def by_tiles(blocks, held, at, turned=False):
    return [
        dot(blocks[b], held.one(b, at), 1, 1 if turned else 0) for b in range(HOLD)
    ]


HELD_REFS = 10


LW, LQ, LV, LP, LC, LEND = 0, 128, 256, 384, 512, 768


def leaf_start_kernel(
    src, w, p, q, c, piv, tl, ranks_l, ranks_m, ranks_u, ranks_r,
    first, y0, plan, rows, hold,
):
    b = src[...]
    y = mm(b, w[...])
    v = q[:, TILE:]
    first[0:RHS, :] = mm(b, q[:, 0:TILE])
    first[RHS : 2 * RHS, :] = mm(y, v)
    first[2 * RHS :, :] = cross(p[...], v)
    y0[...] = y
    dest, label = split_target(tl[...], 13)
    plan[0:1, :] = dest.astype(F32)
    plan[1:2, :] = label
    plan[2:3, :] = leaf_slots(row_onehot(dest, 64))
    plan[3:8, :] = jnp.zeros((5, 2 * TILE), F32)
    found = []
    for ranks, groups, dim in (
        (ranks_l, 1, 1), (ranks_m, 16, 1), (ranks_u, 32, 0), (ranks_r, 64, 0),
    ):
        found += mask_rows(ranks, groups, dim)
    rows[...] = jnp.concatenate(found[0:7] + [piv[...]], axis=0)
    hold[LW:LQ, :] = w[...]
    hold[LQ:LV, :] = q[:, 0:TILE]
    hold[LV:LP, :] = v
    hold[LP:LC, :] = p[...]
    hold[LC:LEND, :] = c[...]


def pack_kernel(*refs):
    (sm, wm, pm, qm, vm, cm, tm), rest = refs[0:7], refs[7:]
    (su, wu, pu, qu, vu, cu, tu), rest = rest[0:7], rest[7:]
    (sr, wr, pr, qr, vr), rest = rest[0:5], rest[5:]
    pack_m, pack_u = rest
    for pack, s, wt, pt, qt, vt, ct, t in (
        (pack_m, sm, wm, pm, qm, vm, cm, tm),
        (pack_u, su, wu, pu, qu, vu, cu, tu),
    ):
        pack[SRC:WAT, :] = s[...]
        pack[WAT:QAT, :] = wt[...]
        pack[QAT:VAT, :] = qt[:, 0:TILE]
        pack[VAT:MISC, :] = qt[:, TILE:]
        at = iota((8, TILE), 0)
        pack[MISC:CAT, :] = jnp.where(
            at == 0,
            jnp.broadcast_to(vt[...], (8, TILE)),
            jnp.broadcast_to(t[...].astype(F32), (8, TILE)),
        )
        pack[CAT:PAT, :] = ct[...]
        pack[PAT:END, :] = pt[...]
    pack_u[END + SRC : END + WAT, :] = sr[...]
    pack_u[END + WAT : END + QAT, :] = wr[...]
    pack_u[END + QAT : END + RMISC, :] = qr[:, 0:TILE]
    pack_u[END + RMISC : END + RPAT, :] = jnp.broadcast_to(vr[...], (8, TILE))
    pack_u[END + RPAT : END + REND, :] = pr[...]


def cross_kernel(*refs):
    _, k1, k2, low, high, low_core, high_core = refs[HELD_REFS:]
    for source, kept in zip(refs[3:5] + refs[8:10], (low, high, low_core, high_core)):
        kept[...] = source[...]
    upper = Held(refs, END)
    root = Held(refs, END, END)
    k1[...] = cross(upper.all(PAT), upper.all(VAT))
    total = None
    for b in range(HOLD):
        p = root.one(b, RPAT)
        part = mm(p.T * root.one(b, RMISC, 1), p)
        total = part if total is None else total + part
    k2[...] = total


def leaf_picks(plan):
    dest = plan[0:1, :].astype(jnp.int32)
    place = lax.shift_right_logical(dest, 3) * 4 + jnp.bitwise_and(dest, 3)
    half = jnp.bitwise_and(lax.shift_right_logical(dest, 2), 1)
    hit = row_onehot(place, 4 * HOLD)
    return [hit * (half == h).astype(F32) for h in range(2)]


def leaf_up_kernel(s0, s1, s2, s3, y0, plan, rows, hold, out, z_out, zp_out, k_out):
    total = (s0[...] + s1[...]) + (s2[...] + s3[...])
    mh, mc = masks(rows, 0)
    k1 = total[2 * RHS :, :]
    hq = total[0:RHS, :] * mh
    wv = (total[RHS : 2 * RHS, :] + mm(hq, k1)) * mc
    e = -mmt(wv, hold[LC:LEND, :])
    both = jnp.concatenate([e, label_rows(plan[1:2, :])], axis=0)
    at = plan[2:3, :]
    parts = jnp.concatenate(
        [both * (at == float(k)).astype(F32) for k in range(SLOTS_LEAF)], axis=0
    )
    both = stacked(parts)
    sent = tall([fold(raw(both, pick.astype(BF16), 1, 1)) for pick in leaf_picks(plan)]).T
    for place in range(0, HOLD, 2):
        pairs = [sent[4 * at : 4 * at + 4, :] for at in (place, place + 1)]
        for at, part in zip((place, place + 1), pairs):
            twice = jnp.concatenate([part, part], axis=0)
            for copy in range(0, HOLD, 2):
                low = (at * HOLD + copy) * 4
                out[low : low + HOLD, :] = twice
    p = hold[LP:LC, :]
    z = (y0[...] + mmt(hq, p)) * rows[7:8, :]
    z_out[...] = z
    zp_out[...] = mm(z, p)
    k_out[...] = k1


def write_copies(ref, value):
    rows = value.shape[0]
    for i in range(ref.shape[0] // rows):
        ref[rows * i : rows * (i + 1), :] = value


def write_shares(ref, members, value, parts):
    step = ref.shape[0] // members
    rows = step - parts.shape[0] // min(members, 16)
    each = step - rows
    common = value.shape[0] == rows
    for i in range(members):
        low = step * i
        ref[low : low + rows, :] = value if common else value[rows * i : rows * (i + 1)]
        at = each * (i % 16)
        ref[low + rows : low + step, :] = parts[at : at + each]


def sum_rows(ref, step, low, high):
    total = ref[low:high, :]
    for i in range(1, ref.shape[0] // step):
        total = total + ref[step * i + low : step * i + high, :]
    return total


def stack_rows(ref, step, low, high, count):
    return jnp.concatenate(
        [ref[step * i + low : step * i + high, :] for i in range(count)], axis=0
    )


def enter_middle_kernel(*refs):
    got, part, y_out, upd_out, scratch, sems = refs[HELD_REFS:]
    held = Fetched(refs, MISC, SRC, VAT, scratch, sems)
    inc = received(got[...].T, True, 2 * TILE)
    held.wait()
    b = [held.one(j, SRC, RHS) + inc[RHS * j : RHS * (j + 1), 0:TILE] for j in range(HOLD)]
    write_copies(part, mm(lanes(b), held.all(QAT)))
    y_out[...] = lanes(by_tiles(b, held, WAT))
    upd_out[...] = inc[:, TILE:]


def middle_kernel(*refs):
    red, y0, rows, part, z_out, zp_out, scratch, sems = refs[HELD_REFS:]
    held = Fetched(refs, MISC, VAT, END, scratch, sems)
    mh, _ = masks(rows, 1)
    hq = sum_rows(red, RHS, 0, RHS) * mh
    held.wait()
    p, v = held.all(PAT), held.all(VAT)
    y = y0[...] + mmt(hq, p)
    write_shares(part, 8, mm(y, v), cross(p, v))
    z = y * lanes([held.one(b, MISC, 1) for b in range(HOLD)])
    z_out[...] = z
    zp_out[...] = mm(z, p)


def middle_up_kernel(*refs):
    red, upd, rows, k1, out, k_out, scratch, copied, sems = refs[HELD_REFS:]
    held = Fetched(refs, MISC, MISC, PAT, copied, sems)
    _, mc = masks(rows, 1)
    total = sum_rows(red, 3 * RHS, 0, 3 * RHS)
    k_out[...] = total[RHS:, :]
    wv = total[0:RHS, :] * mc
    held.wait()
    e = cut_lanes(mmt(wv, held.all(CAT)))
    upds = cut_tall(upd[...])
    targets = held.misc(MISC, 1).astype(jnp.int32)
    sent = messages([u - v for u, v in zip(upds, e)], targets, 14, 128, scratch)
    write_shares(out, 16, sent, k1[...])


def enter_upper_kernel(*refs):
    got, part, y_out, upd_out = refs[HELD_REFS:]
    held = Held(refs, END)
    k1 = sum_rows(got, 2 * RHS, RHS, 2 * RHS)
    inc = received(stack_rows(got, 2 * RHS, 0, RHS, 16).T, False, 2 * TILE)
    b = [held.one(j, SRC, RHS) + inc[RHS * j : RHS * (j + 1), 0:TILE] for j in range(HOLD)]
    y = lanes(by_tiles(b, held, WAT))
    write_copies(part, tall([mm(lanes(b), held.all(QAT)), mm(y, held.all(VAT)), k1]))
    y_out[...] = y
    upd_out[...] = inc[:, TILE:]


def upper_up_kernel(*refs):
    red, y0, upd, rows, k2, out, z_out, zp_out, k_out, scratch = refs[HELD_REFS:]
    held = Held(refs, END)
    total = sum_rows(red, 3 * RHS, 0, 2 * RHS)
    k1 = stack_rows(red, 3 * RHS, 2 * RHS, 3 * RHS, 16)
    k_out[...] = k1
    mh, mc = masks(rows, 2)
    hq = total[0:RHS, :] * mh
    wv = (total[RHS:, :] + mm(hq, k1)) * mc
    e = cut_lanes(mmt(wv, held.all(CAT)))
    upds = cut_tall(upd[...])
    targets = held.misc(MISC, 1).astype(jnp.int32)
    sent = messages([u - v for u, v in zip(upds, e)], targets, 15, 256, scratch)
    write_shares(out, 32, sent, k2[...])
    p = held.all(PAT)
    y = y0[...] + mmt(hq, p)
    z = y * lanes([held.one(b, MISC, 1) for b in range(HOLD)])
    z_out[...] = z
    zp_out[...] = mm(z, p)


def enter_root_kernel(*refs):
    got, part, y_out = refs[HELD_REFS:]
    held = Held(refs, END, END)
    k2 = sum_rows(got, 2 * RHS, RHS, 2 * RHS)
    inc = received(stack_rows(got, 2 * RHS, 0, RHS, 32).T, False, TILE)
    b = [held.one(j, SRC, RHS) + inc[RHS * j : RHS * (j + 1)] for j in range(HOLD)]
    y = lanes(by_tiles(b, held, WAT))
    z = y * lanes([held.one(j, RMISC, 1) for j in range(HOLD)])
    write_copies(part, tall([mm(lanes(b), held.all(QAT)), mm(z, held.all(RPAT)), k2]))
    y_out[...] = y


def root_kernel(*refs):
    red, y0, rows, got, answer, reply = refs[HELD_REFS:]
    held = Held(refs, END, END)
    total = sum_rows(red, 3 * RHS, 0, 2 * RHS)
    k2 = stack_rows(red, 3 * RHS, 2 * RHS, 3 * RHS, 16)
    mh = rows[6:7, :]
    hq = total[0:RHS, :] * mh
    pr = (total[RHS:, :] + mm(hq, k2)) * mh
    turned = stack_rows(got, 2 * RHS, 0, RHS, 32).T
    r = y0[...] + mmt(hq, held.all(RPAT))
    r = r * lanes([held.one(j, RMISC, 1) for j in range(HOLD)])
    x = by_tiles(cut_lanes(r), held, WAT, True)
    low = cut_lanes(mmt(pr, held.all(QAT)))
    x = [u + v for u, v in zip(x, low)]
    answer[...] = x[0]
    reply[...] = replies(turned, False, tall(x))


def fetch_kernel(shift, cut, *refs):
    back, *tails, part, xu_out, scratch = refs[HELD_REFS:]
    held = Held(refs, cut)
    targets = held.misc(MISC, 1).astype(jnp.int32)
    xu = fetched(back[...], targets, shift, scratch)
    write_copies(part, tall([mm(lanes(xu), held.all(CAT))] + [ref[...] for ref in tails]))
    xu_out[...] = tall(xu)


def solve_held(total, z, k1, held, mh, mc):
    s = total[0:RHS, :] * mc
    r = z - mmt(s, held.all(VAT))
    pr = (total[RHS:, :] - mmt(s, k1)) * mh
    x = by_tiles(cut_lanes(r), held, WAT, True)
    low = cut_lanes(mmt(pr, held.all(QAT)))
    return [u + v for u, v in zip(x, low)]


def down_upper_kernel(*refs):
    red, z, rows, xu, got, k1, answer, reply = refs[HELD_REFS:]
    held = Held(refs, END)
    mh, mc = masks(rows, 2)
    total = sum_rows(red, 2 * RHS, 0, 2 * RHS)
    turned = stack_rows(got, 2 * RHS, 0, RHS, 16).T
    x = solve_held(total, z[...], k1[...], held, mh, mc)
    answer[...] = x[0]
    reply[...] = replies(turned, False, jnp.concatenate([tall(x), xu[...]], axis=1))


def down_middle_kernel(*refs):
    red, z, rows, xu, got, answer, reply = refs[HELD_REFS:]
    held = Held(refs, MISC)
    mh, mc = masks(rows, 1)
    total = sum_rows(red, 4 * RHS, 0, 2 * RHS)
    k1 = stack_rows(red, 4 * RHS, 2 * RHS, 4 * RHS, 8)
    me = own_number()
    pair = lax.shift_right_logical(me, 1)
    odd = jnp.bitwise_and(me, 1) == 1
    asked = []
    for i in range(HOLD):
        two = got[pl.ds(pl.multiple_of((4 * i + pair) * HOLD, HOLD), HOLD), :]
        asked.append(jnp.where(odd, two[4:], two[0:4]))
    x = solve_held(total, z[...], k1, held, mh, mc)
    answer[...] = x[0]
    both = jnp.concatenate([tall(x), xu[...]], axis=1)
    reply[...] = replies(tall(asked).T, True, both)


def fetch_leaf_kernel(back, plan, hold, zp, part):
    turned = back[...].T
    both = None
    for h, pick in enumerate(leaf_picks(plan)):
        first = h * SLOTS_LEAF
        slots = tall(
            [turned[SLOT * k : SLOT * k + RHS, :] for k in range(first, first + SLOTS_LEAF)]
        )
        one = fold(raw(stacked(slots), pick.astype(BF16), 1, 0))
        both = one if both is None else both + one
    at = plan[2:3, :]
    xu = None
    for k in range(SLOTS_LEAF):
        one = both[RHS * k : RHS * (k + 1), :] * (at == float(k)).astype(F32)
        xu = one if xu is None else xu + one
    part[0:RHS, :] = mm(xu, hold[LC:LEND, :])
    part[RHS:, :] = zp[...]


def leaf_kernel(s0, s1, s2, s3, z, k1, hold, rows, answer):
    total = (s0[...] + s1[...]) + (s2[...] + s3[...])
    mh, mc = masks(rows, 0)
    s = total[0:RHS, :] * mc
    r = z[...] - mmt(s, hold[LV:LP, :])
    pr = (total[RHS:, :] - mmt(s, k1[...])) * mh
    answer[...] = mmt(r, hold[LW:LQ, :]) + mmt(pr, hold[LQ:LV, :])


def run(kernel, shapes, *args, answer=False, inputs=False, scratch=(), copied=0):
    outs = [pltpu.VMEM(s, F32) for s in shapes]
    if answer:
        outs[0] = jax.ShapeDtypeStruct(shapes[0], F32)
    options = {}
    scratch = [pltpu.VMEM(s, F32) for s in scratch]
    if copied:
        scratch += [pltpu.VMEM((HOLD, copied, TILE), F32), pltpu.SemaphoreType.DMA((12,))]
        rest = [pltpu.with_memory_space_constraint(a, pltpu.VMEM) for a in args[HELD_REFS:]]
        far = [pltpu.with_memory_space_constraint(a, pltpu.HBM) for a in args[:HELD_REFS]]
        args = far + rest
        options["in_specs"] = [pl.BlockSpec(memory_space=pltpu.HBM)] * HELD_REFS + [
            pl.BlockSpec(memory_space=pltpu.VMEM) for _ in rest
        ]
    elif not inputs:
        args = [pltpu.with_memory_space_constraint(a, pltpu.VMEM) for a in args]
    return pl.pallas_call(
        kernel,
        out_shape=outs[0] if len(outs) == 1 else outs,
        scratch_shapes=scratch,
        compiler_params=None if inputs else pltpu.CompilerParams(vmem_limit_bytes=16 << 20),
        **options,
    )(*args)


def after(done, *values):
    return lax.optimization_barrier((*values, done))[:-1]


def swap(value, axis, mask):
    pairs = [(s, s ^ mask) for s in range(lax.axis_size(axis))]
    return lax.ppermute(value, axis, pairs)


def shift(value, step):
    size = lax.axis_size("grid")
    return lax.ppermute(value, "grid", [(s, (s + step) % size) for s in range(size)])


def four(value, axis, unit):
    return [value] + [swap(value, axis, unit * m) for m in (1, 2, 3)]


def together(*values):
    return lax.optimization_barrier(values)


def between(value, members):
    size = lax.axis_size("leaf")
    groups = [
        [start + core + 2 * i for i in range(members)]
        for start in range(0, size, 2 * members)
        for core in range(2)
    ]
    return lax.all_to_all(
        value, "leaf", split_axis=0, concat_axis=0, tiled=True, axis_index_groups=groups
    )


def route_leaf(value):
    size = lax.axis_size("leaf") * lax.axis_size("grid")
    groups = [list(range(g, g + 64)) for g in range(0, size, 64)]
    return lax.all_to_all(
        value,
        ("leaf", "grid"),
        split_axis=0,
        concat_axis=0,
        tiled=True,
        axis_index_groups=groups,
    )


def shards(
    src_l, w_l, p_l, q_l, piv_l, c_l, ranks_l, t_l,
    src_m, w_m, p_m, q_m, piv_m, c_m, ranks_m, t_m,
    src_u, w_u, p_u, q_u, piv_u, c_u, ranks_u, t_u,
    src_r, w_r, p_r, q_r, piv_r, ranks_r,
):
    ranks_l, ranks_m = ranks_l.T, ranks_m.T
    t_l, t_m, t_u = (t.reshape(1, -1) for t in (t_l, t_m, t_u))
    piv_l, piv_m, piv_u, piv_r = (v.reshape(1, -1) for v in (piv_l, piv_m, piv_u, piv_r))
    row = (RHS, TILE)
    pair = (2 * RHS, TILE)
    flat = (RHS, HOLD * TILE)
    high = (HOLD * RHS, TILE)

    first, y_l, plan, rows, hold = run(
        leaf_start_kernel,
        [(2 * RHS + TILE, TILE), row, (RHS, 2 * TILE), row, (LEND, TILE)],
        src_l, w_l, p_l, q_l, c_l, piv_l, t_l, ranks_l, ranks_m, ranks_u, ranks_r,
        inputs=True,
    )
    sums = four(first, "grid", 1)
    pack_m, pack_u = run(
        pack_kernel, [(END, TILE), (END + REND, TILE)],
        src_m, w_m, p_m, q_m, piv_m, c_m, t_m,
        src_u, w_u, p_u, q_u, piv_u, c_u, t_u,
        src_r, w_r, p_r, q_r, piv_r,
        inputs=True,
    )
    m_core, u_core = swap(pack_m, "leaf", 1), swap(pack_u, "leaf", 1)
    *sums, pack_m = together(*sums, pack_m)
    m_prev = shift(pack_m, 1)
    m_next = shift(pack_m, -1)
    out, z_l, zp_l, k_l = run(
        leaf_up_kernel,
        [(64 * 4, LANES), row, row, (TILE, TILE)],
        *sums, y_l, plan, rows, hold,
    )
    got_m = route_leaf(out)
    m_prev, m_next, pack_u = after(got_m, m_prev, m_next, pack_u)
    m_low, m_high = shift(m_prev[:MISC], 1), shift(m_next[MISC:], -1)
    m_prev_core, m_next_core = swap(m_prev, "leaf", 1), swap(m_next, "leaf", 1)
    u_prev, u_next = shift(pack_u, 1), shift(pack_u, -1)
    m_low_core, m_high_core = swap(m_low, "leaf", 1), swap(m_high, "leaf", 1)
    held_m = (
        pack_m, m_prev, m_next, m_low, m_high,
        m_core, m_prev_core, m_next_core, m_low_core, m_high_core,
    )

    part, y_m, upd_m = run(
        enter_middle_kernel, [(8 * RHS, TILE), flat, high], *held_m, got_m,
        copied=VAT - SRC,
    )
    red = between(part, 8)
    u_prev, u_next = after(red, u_prev, u_next)
    u_low, u_high = shift(u_prev[:END], 1), shift(u_next[END:], -1)
    u_prev_core, u_next_core = swap(u_prev, "leaf", 1), swap(u_next, "leaf", 1)
    part, z_m, zp_m = run(
        middle_kernel, [(8 * 3 * RHS, TILE), flat, row], *held_m, red, y_m, rows,
        copied=END - VAT,
    )
    u_low, u_high = after(part, u_low, u_high)
    held_u = (
        pack_u, u_prev, u_next, u_low, u_high,
        u_core, u_prev_core, u_next_core, swap(u_low, "leaf", 1), swap(u_high, "leaf", 1),
    )
    red = between(part, 8)
    k_u, k_r, *opposite = run(
        cross_kernel, [(TILE, TILE)] * 2 + [(END, TILE), (REND, TILE)] * 2, *held_u, red
    )
    held_u = (*held_u[:3], *opposite[:2], *held_u[5:8], *opposite[2:])
    out, k_m = run(
        middle_up_kernel, [(16 * 2 * RHS, LANES), pair],
        *held_m, red, upd_m, rows, k_u, scratch=[(LANES, 128)], copied=PAT - MISC,
    )
    got_u = between(out, 16)

    part, y_u, upd_u = run(
        enter_upper_kernel, [(16 * 3 * RHS, TILE), flat, high], *held_u, got_u
    )
    red = between(part, 16)
    out, z_u, zp_u, k_u = run(
        upper_up_kernel, [(32 * 2 * RHS, LANES), flat, row, (TILE, TILE)],
        *held_u, red, y_u, upd_u, rows, k_r, scratch=[(LANES, 256)],
    )
    got_r = between(out, 32)

    part, y_r = run(enter_root_kernel, [(32 * 3 * RHS, TILE), flat], *held_u, got_r)
    red = between(part, 32)
    x_r, out = run(
        root_kernel, [row, (256, LANES)], *held_u, red, y_r, rows, got_r, answer=True
    )

    back = between(out, 32)
    part, xu = run(
        functools.partial(fetch_kernel, 15, END), [(16 * 2 * RHS, TILE), high],
        *held_u, back, zp_u, scratch=[(LANES, 256)],
    )
    red = between(part, 16)
    x_u, out = run(
        down_upper_kernel, [row, (128, LANES)],
        *held_u, red, z_u, rows, xu, got_u, k_u, answer=True,
    )

    back = between(out, 16)
    part, xu = run(
        functools.partial(fetch_kernel, 14, MISC), [(8 * 4 * RHS, TILE), high],
        *held_m, back, zp_m, k_m, scratch=[(LANES, 128)],
    )
    red = between(part, 8)
    x_m, out = run(
        down_middle_kernel, [row, (32, LANES)],
        *held_m, red, z_m, rows, xu, got_m, answer=True,
    )

    back = between(out, 8)
    part = run(fetch_leaf_kernel, [pair], back, plan, hold, zp_l)
    x_l = run(leaf_kernel, [row], *four(part, "grid", 1), z_l, k_l, hold, rows, answer=True)
    return (x_l, x_m, x_u, x_r)


def solution(mesh):
    both = ("leaf", "grid")
    wide = P(None, both)
    deep = P(both, None)
    line = P(both)
    level = (wide, deep, deep, deep, line, deep, P(), line)
    in_specs = level * 3 + (wide, deep, deep, deep, line, P())
    return jax.shard_map(
        shards, mesh=mesh, in_specs=in_specs, out_specs=(wide,) * 4, check_vma=False
    )
```
